32 devices in a mesh: row: 4 (over y, x), col: 8 (over z, core).
Axes of the slice: x: 2, y: 2, z: 4, core: 2. Of those that a mesh axis runs over, the one named last changes fastest.
Arguments:
- pair: float32 [256, 256, 128], P('row', 'col'), may hold values from -6 to 6
- valid_length: int32 [1], replicated, may hold values from 64 to 255
- tri_in: bfloat16 [128, 512], replicated, may hold values from -0.5 to 0.5
- tri_gate: bfloat16 [128, 128], replicated, may hold values from -0.5 to 0.5
- tri_out: bfloat16 [128, 128], replicated, may hold values from -0.5 to 0.5
- att_in: bfloat16 [128, 512], replicated, may hold values from -16.9705627 to 16.9705627
- att_bias: bfloat16 [128, 4], replicated, may hold values from -0.5 to 0.5
- att_out: bfloat16 [128, 128], replicated, may hold values from -0.5 to 0.5
Outputs:
- pair_out: float32 [256, 256, 128], P('row', 'col')
The draws below stay inside these ranges and needn't reach their ends.
Inputs may be any that keep to these rules, and one draw needn't show every extreme that they name: Tokens at positions below valid_length[0] are real, the rest are padding.
All inputs are finite; a program needn't handle non-finite values.
Results may differ from the reference program's by a relative error of at most 0.025.
Values may be sent and summed in bfloat16 or wider, within the bound.
No kernel may reach another device: no remote copies, remote signals or barrier semaphores. Data moves between devices by JAX's collectives and lax.ppermute only.
A program may use at most 128 MiB of HBM per device.

```python
import jax
import jax.numpy as jnp
from jax import lax

C = 128
CH = 128
H = 4
DH = 32
N = 256


def draw_att_in(key, part):
    raw = jax.random.truncated_normal(key, -4.0, 4.0, (C, 4 * C), jnp.float32) * C ** (-0.5)
    return raw.astype(jnp.bfloat16)


def shard_levels(stream_key, dims, shards, least, largest):
    factor_of, own = 1.0, jax.random.fold_in(stream_key, 6)
    for dim, shards_of in shards:
        heights = jnp.exp(jax.random.uniform(jax.random.fold_in(own, dim), (shards_of,), jnp.float32, least / len(shards), largest / len(shards)))
        factor_of = factor_of * jnp.repeat(heights, dims[dim] // shards_of).reshape([-1 if axis == dim else 1 for axis in range(len(dims))])
    return factor_of


def noise(key, extent, width, most, shards=(), held_as=jnp.bfloat16):
    array = width * jax.random.normal(key, extent, jnp.float32)
    if shards:
        array = array * shard_levels(key, extent, shards, -0.22, 0.18)
    return jnp.clip(array, -most, most).astype(held_as)


def setup_inputs(seed: int = 0) -> dict:
    splits = jax.random.split(jax.random.key(seed), 9)
    return {
        "pair": noise(splits[0], (N, N, C), 1.0, 6.0, ((0, 4), (1, 8)), jnp.float32),
        "valid_length": jax.random.randint(splits[1], (1,), N // 4, N).astype(jnp.int32),
        "tri_in": noise(splits[2], (C, 4 * CH), C ** -0.5, 0.5),
        "tri_gate": noise(splits[3], (C, C), C ** -0.5, 0.5),
        "tri_out": noise(splits[4], (CH, C), CH ** -0.5, 0.5),
        "att_in": draw_att_in(jax.random.fold_in(splits[8], 71), 0),
        "att_bias": noise(splits[6], (C, H), C ** -0.5, 0.5),
        "att_out": noise(splits[7], (C, C), C ** -0.5, 0.5),
    }


def layer_norm(values):
    center = values - lax.optimization_barrier(jnp.mean(values, axis=-1, keepdims=True))
    return center * lax.rsqrt(lax.optimization_barrier(jnp.mean(center * center, axis=-1, keepdims=True)) + 1e-05)

def reference(pair, valid_length, tri_in, tri_gate, tri_out, att_in, att_bias, att_out):
    tokens = jnp.arange(N).astype(jnp.int32)
    keep = (tokens < valid_length[0]).astype(jnp.float32)
    blocks = N // 8
    normed_pair = layer_norm(pair).astype(jnp.bfloat16)

    def edges(packed):
        rows, row_keep = packed
        projected = jnp.dot(rows, tri_in, preferred_element_type=jnp.float32)
        weight = (row_keep[:, None] * keep[None, :])[:, :, None]
        left = jax.nn.sigmoid(projected[..., :CH]) * projected[..., CH:2 * CH] * weight
        right = jax.nn.sigmoid(projected[..., 2 * CH:3 * CH]) * projected[..., 3 * CH:] * weight
        return (left.astype(jnp.bfloat16), right.astype(jnp.bfloat16))
    left_edges, right_edges = lax.map(edges, (normed_pair.reshape(blocks, 8, N, C), keep.reshape(blocks, 8)))
    left_edges = left_edges.reshape(N, N, CH)
    right_edges = right_edges.reshape(N, N, CH)
    products = jnp.einsum('ikc,jkc->ijc', left_edges.astype(jnp.float32), right_edges.astype(jnp.float32))
    normed_products = layer_norm(products).astype(jnp.bfloat16)
    update = jax.nn.sigmoid(jnp.dot(normed_pair, tri_gate, preferred_element_type=jnp.float32)) * jnp.dot(normed_products, tri_out, preferred_element_type=jnp.float32)
    middle = pair + update
    normed_mid = layer_norm(middle).astype(jnp.bfloat16)
    bias_all = jnp.dot(normed_mid, att_bias, preferred_element_type=jnp.float32).astype(jnp.bfloat16)
    bias_heads = jnp.transpose(bias_all.astype(jnp.float32), (2, 0, 1))
    mask_bias = jnp.where(tokens < valid_length[0], 0.0, -1000000000.0).astype(jnp.float32)

    def attend(packed):
        block_mid, block_norm = packed
        projected = jnp.dot(block_norm, att_in, preferred_element_type=jnp.float32)
        query = (projected[..., :C] * DH ** (-0.5)).astype(jnp.bfloat16).reshape(8, N, H, DH)
        keys = projected[..., C:2 * C].astype(jnp.bfloat16).reshape(8, N, H, DH)
        values = projected[..., 2 * C:3 * C].astype(jnp.bfloat16).reshape(8, N, H, DH)
        gate = jax.nn.sigmoid(projected[..., 3 * C:])
        scores = jnp.einsum('ijhd,ikhd->ihjk', query.astype(jnp.float32), keys.astype(jnp.float32))
        scores = scores + bias_heads[None] + mask_bias[None, None, None, :]
        weights = jax.nn.softmax(scores, axis=-1)
        attended = jnp.einsum('ihjk,ikhd->ijhd', weights, values.astype(jnp.float32)).reshape(8, N, C)
        gated = (gate * attended).astype(jnp.bfloat16)
        return block_mid + jnp.dot(gated, att_out, preferred_element_type=jnp.float32)
    result = lax.map(attend, (middle.reshape(blocks, 8, N, C), normed_mid.reshape(blocks, 8, N, C)))
    return result.reshape(N, N, C)
```

```python
import functools
import math

import jax
import jax.numpy as jnp
from jax import lax
from jax.experimental import pallas as pl
from jax.experimental.pallas import tpu as pltpu
from jax.sharding import PartitionSpec as P

BF = jnp.bfloat16
F32 = jnp.float32
LOG2E = 1.4426950408889634
NT = (((1,), (1,)), ((), ()))
TN = (((0,), (0,)), ((), ()))
NN = (((1,), (0,)), ((), ()))


def mm(a, b, dims):
    return lax.dot_general(a, b, dims, preferred_element_type=F32)


def sigmoid(v):
    return 0.5 * jnp.tanh(0.5 * v) + 0.5


def layer_norm(v, axis=-1):
    center = v - jnp.mean(v, axis=axis, keepdims=True)
    return center * lax.rsqrt(jnp.mean(center * center, axis=axis, keepdims=True) + 1e-05)


def edges_kernel(valid_ref, start_ref, x_ref, w_ref, out_ref, acc_ref):
    blocks, own, cols, width = x_ref.shape
    total = blocks * cols
    half = w_ref.shape[0] // 2
    keep_k = (lax.broadcasted_iota(jnp.int32, (1, total), 1) < valid_ref[0]).astype(F32)

    for i in range(own):
        x = x_ref[:, i].reshape(total, width).astype(F32)
        normed = layer_norm(x).astype(BF)
        keep_i = jnp.where(start_ref[0] + i < valid_ref[0], 1.0, 0.0).astype(F32)
        weight = keep_k * keep_i
        proj = mm(w_ref[...], normed, NT)
        edge = sigmoid(proj[:half]) * proj[half:] * weight
        for t in range(total // 128):
            acc_ref[t, pl.ds(i, half, stride=own), :] = edge[:, t * 128 : (t + 1) * 128]
    for t in range(total // 128):
        out_ref[:, t * 128 : (t + 1) * 128] = acc_ref[t].astype(BF)


def product_kernel(e_ref, out_ref):
    count, _, _, own, total = e_ref.shape
    left = e_ref[:, 0, 0].astype(F32).reshape(count * own, total).astype(BF)
    right = e_ref[:, 1, 0].astype(F32).reshape(count * own, total).astype(BF)
    prod = mm(left, right, NT)
    out_ref[:, 0] = prod.reshape(count, own, total).astype(BF)


def middle_kernel(p_ref, x_ref, gate_ref, tri_ref, bias_ref, upd_ref, nm_ref, b_ref, acc_ref, bacc_ref):
    blocks, own, cols, width = x_ref.shape
    total = blocks * cols
    hidden = tri_ref.shape[0]
    heads = b_ref.shape[0]
    for t in range(total // 128):
        acc_ref[t] = p_ref[:, t * 128 : (t + 1) * 128].astype(F32)
    for i in range(own):
        prod = jnp.concatenate(
            [acc_ref[t, pl.ds(i, hidden, stride=own), :] for t in range(total // 128)], axis=1
        )
        nprod = layer_norm(prod, axis=0).astype(BF)
        tri = mm(nprod, tri_ref[...], TN)
        x = x_ref[:, i].reshape(total, width).astype(F32)
        normed = layer_norm(x).astype(BF)
        update = sigmoid(mm(normed, gate_ref[...], NN)) * tri
        nm = layer_norm(x + update).astype(BF)
        upd_ref[i] = update
        nm_ref[i] = nm
        bias = mm(bias_ref[...], nm, NT)
        for h in range(heads):
            bacc_ref[h, i : i + 1, :] = bias[h : h + 1]
    b_ref[...] = bacc_ref[...].astype(BF)


def attention_kernel(valid_ref, nm_ref, upd_ref, b_ref, wqk_ref, wvg_ref, wo_ref, out_ref, bt_ref):
    count, heads, own, total = b_ref.shape
    width = wo_ref.shape[0]
    size = width // heads

    @pl.when(pl.program_id(0) == 0)
    def _():
        keep = lax.broadcasted_iota(jnp.int32, (total, 1), 0) < valid_ref[0]
        mask = jnp.where(keep, 0.0, -1000000000.0 * LOG2E).astype(F32)
        for h in range(heads):
            b = b_ref[:, h].astype(F32).reshape(count * own, total)
            bt_ref[h] = jnp.transpose(b) * LOG2E + mask

    nm = nm_ref[0]
    qk = mm(nm, wqk_ref[...], NN)
    query = (qk[:, :width] * (LOG2E * size ** (-0.5))).astype(BF)
    keys = qk[:, width:].astype(BF)
    vg = mm(wvg_ref[...], nm, NT)
    values = vg[:width].astype(BF)
    lane = lax.broadcasted_iota(jnp.int32, (1, width), 1) // size
    outs = []
    for h in range(heads):
        q = jnp.where(lane == h, query, jnp.zeros_like(query))
        s = mm(keys, q, NT) + bt_ref[h]
        p = jnp.exp2(s - jnp.max(s, axis=0, keepdims=True))
        norm = 1.0 / jnp.sum(p, axis=0, keepdims=True)
        o = mm(values[h * size : (h + 1) * size], p.astype(BF), NN)
        outs.append(o * norm)
    gated = (jnp.concatenate(outs, axis=0) * sigmoid(vg[width:])).astype(BF)
    delta = upd_ref[0] + mm(gated, wo_ref[...], TN)
    blocks, _, cols, _ = out_ref.shape
    out_ref[:, 0] = delta.reshape(blocks, cols, width).astype(BF)


VMEM = pl.BlockSpec(memory_space=pltpu.VMEM)
SMEM = pl.BlockSpec(memory_space=pltpu.SMEM)


def cost(flops, nbytes):
    return pl.CostEstimate(flops=flops, bytes_accessed=nbytes, transcendentals=0)


def fast_edges(valid, start, x, weights):
    blocks, own, cols, width = x.shape
    total = blocks * cols
    rows = weights.shape[0] // 2 * own
    return pl.pallas_call(
        edges_kernel,
        out_shape=jax.ShapeDtypeStruct((rows, total), BF),
        in_specs=[SMEM, SMEM, VMEM, VMEM],
        out_specs=VMEM,
        scratch_shapes=[pltpu.VMEM((total // 128, rows, 128), F32)],
        name="edges",
    )(valid, start, x, weights)


def fast_products(edges):
    count, _, chans, own, total = edges.shape
    return pl.pallas_call(
        product_kernel,
        out_shape=jax.ShapeDtypeStruct((count, chans, own, total), BF),
        grid=(chans,),
        in_specs=[pl.BlockSpec((count, 2, 1, own, total), lambda c: (0, 0, c, 0, 0))],
        out_specs=pl.BlockSpec((count, 1, own, total), lambda c: (0, c, 0, 0)),
        name="products",
    )(edges)


def fast_middle(prod, x, tri_gate, tri_out, bias_w, heads):
    blocks, own, cols, width = x.shape
    total = blocks * cols
    rows = prod.shape[0]
    return pl.pallas_call(
        middle_kernel,
        out_shape=(
            jax.ShapeDtypeStruct((own, total, width), F32),
            jax.ShapeDtypeStruct((own, total, width), BF),
            jax.ShapeDtypeStruct((heads, own, total), BF),
        ),
        in_specs=[VMEM] * 5,
        out_specs=(VMEM,) * 3,
        scratch_shapes=[
            pltpu.VMEM((total // 128, rows, 128), F32),
            pltpu.VMEM((heads, own, total), F32),
        ],
        name="middle",
    )(prod, x, tri_gate, tri_out, bias_w)


def fast_attention(valid, nm, upd, bias, wqk, wvg, wo, cols):
    own, total, width = nm.shape
    count, heads = bias.shape[:2]
    blocks = total // cols
    whole = lambda a: pl.BlockSpec(a.shape, lambda i: (0,) * a.ndim)
    row = pl.BlockSpec((1, total, width), lambda i: (i, 0, 0))
    return pl.pallas_call(
        attention_kernel,
        out_shape=jax.ShapeDtypeStruct((blocks, own, cols, width), BF),
        grid=(own,),
        in_specs=[SMEM, row, row, whole(bias), whole(wqk), whole(wvg), whole(wo)],
        out_specs=pl.BlockSpec((blocks, 1, cols, width), lambda i: (0, i, 0, 0)),
        scratch_shapes=[pltpu.VMEM((heads, total, total), F32)],
        name="attention",
    )(valid, nm, upd, bias, wqk, wvg, wo)


def plain_edges(valid, start, x, weights):
    blocks, own, cols, width = x.shape
    total = blocks * cols
    half = weights.shape[0] // 2
    normed = layer_norm(jnp.swapaxes(x, 0, 1).reshape(own, total, width).astype(F32)).astype(BF)
    proj = jnp.einsum("ec,ikc->eik", weights, normed, preferred_element_type=F32)
    keep_k = (jnp.arange(total) < valid[0]).astype(F32)
    keep_i = (start[0] + jnp.arange(own) < valid[0]).astype(F32)
    edge = sigmoid(proj[:half]) * proj[half:] * (keep_i[:, None] * keep_k[None, :])
    return edge.astype(BF).reshape(half * own, total)


def plain_products(edges):
    count, _, chans, own, total = edges.shape
    flat = jnp.transpose(edges, (1, 2, 0, 3, 4)).reshape(2, chans, count * own, total)
    prod = jnp.einsum("cik,cjk->cij", flat[0], flat[1], preferred_element_type=F32).astype(BF)
    return jnp.transpose(prod.reshape(chans, count, own, total), (1, 0, 2, 3))


def plain_middle(prod, x, tri_gate, tri_out, bias_w, heads):
    blocks, own, cols, width = x.shape
    total = blocks * cols
    prod = prod.reshape(tri_out.shape[0], own, total).astype(F32)
    nprod = layer_norm(prod, axis=0).astype(BF)
    tri = jnp.einsum("cij,cd->ijd", nprod, tri_out, preferred_element_type=F32)
    pair = jnp.swapaxes(x, 0, 1).reshape(own, total, width).astype(F32)
    normed = layer_norm(pair).astype(BF)
    update = sigmoid(jnp.dot(normed, tri_gate, preferred_element_type=F32)) * tri
    nm = layer_norm(pair + update).astype(BF)
    bias = jnp.einsum("hc,ijc->hij", bias_w[:heads], nm, preferred_element_type=F32).astype(BF)
    return update, nm, bias


def plain_attention(valid, nm, upd, bias, wqk, wvg, wo, cols):
    own, total, width = nm.shape
    count, heads = bias.shape[:2]
    size = width // heads
    qk = jnp.dot(nm, wqk, preferred_element_type=F32)
    query = (qk[..., :width] * (LOG2E * size ** (-0.5))).astype(BF).reshape(own, total, heads, size)
    keys = qk[..., width:].astype(BF).reshape(own, total, heads, size)
    vg = jnp.einsum("ec,ijc->ije", wvg, nm, preferred_element_type=F32)
    values = vg[..., :width].astype(BF).reshape(own, total, heads, size)
    table = jnp.swapaxes(bias.astype(F32), 0, 1).reshape(heads, total, total) * LOG2E
    mask = jnp.where(jnp.arange(total) < valid[0], 0.0, -1000000000.0 * LOG2E).astype(F32)

    def one(args):
        q, k, v = args
        s = jnp.einsum("jhd,khd->hjk", q, k, preferred_element_type=F32) + table + mask
        p = jnp.exp2(s - jnp.max(s, axis=-1, keepdims=True))
        o = jnp.einsum("hjk,khd->jhd", p.astype(BF), v, preferred_element_type=F32)
        return o / jnp.transpose(jnp.sum(p, axis=-1))[..., None]

    att = lax.map(one, (query, keys, values)).reshape(own, total, width)
    gated = (sigmoid(vg[..., width:]) * att).astype(BF)
    delta = upd + jnp.dot(gated, wo, preferred_element_type=F32)
    return jnp.swapaxes(delta.astype(BF).reshape(own, total // cols, cols, width), 0, 1)


def per_device(pair, valid_length, tri_in, tri_gate, tri_out, att_in, att_bias, att_out):
    rows_dev, cols_dev, width = pair.shape
    hidden = tri_out.shape[0]
    heads = att_bias.shape[1]
    ncol = lax.axis_size("col")
    ndev = ncol * lax.axis_size("row")
    total = cols_dev * ncol
    own = rows_dev // ncol
    chans = hidden // ndev
    both = ("row", "col")
    start = (lax.axis_index(both) * own).astype(jnp.int32).reshape(1)
    fast = own % 8 == 0 and total % 128 == 0
    edges_of = fast_edges if fast else plain_edges
    products_of = fast_products if fast else plain_products
    middle_of = fast_middle if fast else plain_middle
    attention_of = fast_attention if fast else plain_attention

    parts = jnp.transpose(tri_in).reshape(4, ndev, chans, width)
    gates = jnp.stack([parts[0], parts[2]], axis=1)
    vals = jnp.stack([parts[1], parts[3]], axis=1)
    weights = jnp.concatenate([gates.reshape(-1, width), vals.reshape(-1, width)], axis=0)

    x = lax.all_to_all(pair.astype(BF), "col", 0, 0, tiled=True)
    x = x.reshape(ncol, own, cols_dev, width)
    edges = edges_of(valid_length, start, x, weights)
    edges = edges.reshape(ndev, 2 * chans * own, total)
    edges = lax.all_to_all(edges, both, 0, 0, tiled=True)
    prod = products_of(edges.reshape(ndev, 2, chans, own, total))
    prod = prod.reshape(ndev, chans * own, total)
    prod = lax.all_to_all(prod, both, 0, 0, tiled=True).reshape(hidden * own, total)
    pad = -heads % 8
    bias_w = jnp.pad(jnp.transpose(att_bias), ((0, pad), (0, 0)))
    upd, nm, bias = middle_of(prod, x, tri_gate, tri_out, bias_w, heads)
    bias = lax.all_to_all(
        jnp.broadcast_to(bias[None], (ndev, heads, own, total)), both, 0, 0, tiled=True
    )
    wvg = jnp.transpose(att_in[:, 2 * width :])
    delta = attention_of(
        valid_length, nm, upd, bias, att_in[:, : 2 * width], wvg, att_out, cols_dev
    )
    delta = delta.reshape(rows_dev, cols_dev, width)
    delta = lax.all_to_all(delta, "col", 0, 0, tiled=True)
    return pair + delta.astype(F32)


def solution(mesh):
    placed = (P("row", "col", None), P(), P(), P(), P(), P(), P(), P())
    return jax.shard_map(
        per_device, mesh=mesh, in_specs=placed, out_specs=P("row", "col", None), check_vma=False
    )
```

```python
import functools

import jax
import jax.numpy as jnp
from jax import lax
from jax.experimental import pallas as pl
from jax.experimental.pallas import tpu as pltpu
from jax.sharding import Mesh
from jax.sharding import PartitionSpec as P

BF = jnp.bfloat16
F32 = jnp.float32
LOG2E = 1.4426950408889634
GROUP = 2
NT = (((1,), (1,)), ((), ()))
TN = (((0,), (0,)), ((), ()))
NN = (((1,), (0,)), ((), ()))


def mm(a, b, dims):
    return lax.dot_general(a, b, dims, preferred_element_type=F32)


def sigmoid(v):
    return 0.5 * jnp.tanh(0.5 * v) + 0.5


def layer_norm(v, axis=-1):
    center = v - jnp.mean(v, axis=axis, keepdims=True)
    return center * lax.rsqrt(jnp.mean(center * center, axis=axis, keepdims=True) + 1e-05)


def edge_weights(tri_ref, chans):
    hidden = tri_ref.shape[1] // 4
    new = lax.broadcasted_iota(jnp.int32, (2 * hidden, 2 * hidden), 0)
    old = lax.broadcasted_iota(jnp.int32, (2 * hidden, 2 * hidden), 1)
    side = (new // chans) % 2
    wanted = side * hidden + new // (2 * chans) * chans + new % chans
    pick = jnp.where(old == wanted, 1.0, 0.0).astype(BF)
    tri = [tri_ref[:, n * hidden : (n + 1) * hidden] for n in range(4)]
    gates = mm(pick, jnp.concatenate([tri[0], tri[2]], axis=1), NT)
    vals = mm(pick, jnp.concatenate([tri[1], tri[3]], axis=1), NT)
    return jnp.concatenate([gates, vals], axis=0).astype(BF)


def edges_kernel(valid_ref, x_ref, tri_ref, out_ref, xb_ref, *, chans):
    rows, cols, width = x_ref.shape
    half = out_ref.shape[0]
    step = 16
    span = step * cols
    valid = valid_ref[0]
    row_start = lax.axis_index("row") * rows
    col_start = (lax.axis_index("z") * 2 + lax.axis_index("core")) * cols
    weights = edge_weights(tri_ref, chans)
    token = lax.broadcasted_iota(jnp.int32, (1, span), 1)
    keep_k = (col_start + token % cols < valid).astype(F32)
    for n in range(rows // step):
        x = x_ref[n * step : (n + 1) * step]
        xb_ref[n * step : (n + 1) * step] = x.astype(BF)
        normed = layer_norm(x.reshape(span, width)).astype(BF)
        keep_i = (row_start + n * step + token // cols < valid).astype(F32)
        proj = mm(weights, normed, NT)
        edge = sigmoid(proj[:half]) * proj[half:] * (keep_k * keep_i)
        out_ref[:, n * span : (n + 1) * span] = edge.astype(BF)


def product_kernel(e_ref, out_ref, acc_ref, *, ncol, cols):
    count, both, tokens = e_ref.shape
    chans = both // 2
    quads = ncol // 4
    total = ncol * cols
    rows = tokens // cols
    pitch = acc_ref.shape[1] // both
    lane = lax.broadcasted_iota(jnp.int32, (both, 128), 1)
    low = lane < 64
    even = (lane // 32) % 2 == 0

    def per_row(r, carry):
        for q in range(quads):
            src = [e_ref[r * ncol + q * 4 + g].astype(F32) for g in range(4)]
            for t in range(tokens // 128):
                a = [v[:, t * 128 : (t + 1) * 128] for v in src]
                c = [
                    jnp.where(low, a[0], pltpu.roll(a[2], 64, 1)),
                    jnp.where(low, a[1], pltpu.roll(a[3], 64, 1)),
                    jnp.where(low, pltpu.roll(a[0], 64, 1), a[2]),
                    jnp.where(low, pltpu.roll(a[1], 64, 1), a[3]),
                ]
                d = [
                    jnp.where(even, c[0], pltpu.roll(c[1], 32, 1)),
                    jnp.where(even, pltpu.roll(c[0], 96, 1), c[1]),
                    jnp.where(even, c[2], pltpu.roll(c[3], 32, 1)),
                    jnp.where(even, pltpu.roll(c[2], 96, 1), c[3]),
                ]
                for g in range(4):
                    acc_ref[q, pl.ds(r * rows + t * 4 + g, both, stride=pitch), :] = d[g]
        return carry

    lax.fori_loop(0, count // ncol, per_row, 0)

    def whole(row):
        parts = [acc_ref[q, row * pitch : row * pitch + total, :] for q in range(quads)]
        return jnp.concatenate(parts, axis=1).astype(BF)

    for c in range(chans):
        prod = mm(whole(c), whole(chans + c), NT)
        out_ref[:, c] = prod.reshape(count, total // count, total).astype(BF)


def middle_kernel(p_ref, x_ref, gate_ref, tri_ref, bias_ref, upd_ref, nm_ref, b_ref, acc_ref, bacc_ref):
    blocks, own, cols, width = x_ref.shape
    total = blocks * cols
    hidden = tri_ref.shape[0]
    heads = b_ref.shape[1]
    for t in range(total // 128):
        acc_ref[t] = p_ref[:, t * 128 : (t + 1) * 128].astype(F32)
    for i in range(own):
        prod = jnp.concatenate(
            [acc_ref[t, pl.ds(i, hidden, stride=own), :] for t in range(total // 128)], axis=1
        )
        nprod = layer_norm(prod, axis=0).astype(BF)
        tri = mm(nprod, tri_ref[...], TN)
        x = x_ref[:, i].reshape(total, width).astype(F32)
        normed = layer_norm(x).astype(BF)
        update = sigmoid(mm(normed, gate_ref[...], NN)) * tri
        nm = layer_norm(x + update).astype(BF)
        upd_ref[i] = update
        nm_ref[i] = nm
        bias = mm(bias_ref[...], nm, NT)
        for h in range(heads):
            bacc_ref[h, i : i + 1, :] = bias[h : h + 1]
    bias = bacc_ref[...].astype(BF)
    for n in range(b_ref.shape[0]):
        b_ref[n] = bias


def project_kernel(nm_ref, w_ref, q_ref, k_ref, v_ref, g_ref, *, scale):
    own, total, width = nm_ref.shape
    turned = jnp.transpose(w_ref[:, 2 * width :].astype(F32)).astype(BF)
    for i in range(own):
        nm = nm_ref[i]
        qk = mm(nm, w_ref[:, : 2 * width], NN)
        q_ref[i] = (qk[:, :width] * scale).astype(BF)
        k_ref[i] = qk[:, width:].astype(BF)
        vg = mm(turned, nm, NT)
        v_ref[i] = vg[:width].astype(BF)
        g_ref[i] = sigmoid(vg[width:])


def attention_kernel(
    valid_ref, q_ref, k_ref, v_ref, g_ref, upd_ref, ba_ref, bb_ref, wo_ref, out_ref, bt_ref, tmp_ref, s_ref, p_ref
):
    count, heads, own, total = ba_ref.shape
    width = wo_ref.shape[0]
    size = width // heads
    blocks, _, cols, _ = out_ref.shape
    group = s_ref.shape[0] // heads
    core = lax.axis_index("core")
    keep = lax.broadcasted_iota(jnp.int32, (total, 1), 0) < valid_ref[0]
    mask = jnp.where(keep, 0.0, -1000000000.0 * LOG2E).astype(F32)
    for h in range(heads):
        for n in range(count):
            for ref, side in ((ba_ref, core), (bb_ref, 1 - core)):
                at = pl.multiple_of((2 * n + side) * own, own)
                tmp_ref[h, pl.ds(at, own), :] = ref[n, h].astype(F32)
        bt_ref[h] = jnp.transpose(tmp_ref[h]) * LOG2E + mask
    lane = lax.broadcasted_iota(jnp.int32, (1, width), 1) // size

    def per_group(n, carry):
        tops = []
        norms = []
        for r in range(group):
            query = q_ref[n * group + r]
            for h in range(heads):
                q = jnp.where(lane == h, query, jnp.zeros_like(query))
                s = mm(k_ref[n * group + r], q, NT) + bt_ref[h]
                s_ref[r * heads + h] = s
                tops.append(jnp.max(s, axis=0, keepdims=True))
        for at in range(group * heads):
            p = jnp.exp2(s_ref[at] - tops[at])
            norms.append(1.0 / jnp.sum(p, axis=0, keepdims=True))
            p_ref[at] = p.astype(BF)
        for r in range(group):
            i = n * group + r
            outs = []
            for h in range(heads):
                at = r * heads + h
                outs.append(mm(v_ref[i, h * size : (h + 1) * size], p_ref[at], NN) * norms[at])
            gated = (jnp.concatenate(outs, axis=0) * g_ref[i]).astype(BF)
            delta = upd_ref[i] + mm(gated, wo_ref[...], TN)
            out_ref[:, pl.ds(i, 1)] = delta.reshape(blocks, 1, cols, width).astype(BF)
        return carry

    lax.fori_loop(0, own // group, per_group, 0)


VMEM = pl.BlockSpec(memory_space=pltpu.VMEM)
SMEM = pl.BlockSpec(memory_space=pltpu.SMEM)


def cost(flops, nbytes):
    return pl.CostEstimate(flops=flops, bytes_accessed=nbytes, transcendentals=0)


def fast_edges(valid, pair, tri_in, chans):
    rows, cols, width = pair.shape
    half = tri_in.shape[1] // 2
    return pl.pallas_call(
        functools.partial(edges_kernel, chans=chans),
        out_shape=(
            jax.ShapeDtypeStruct((half, rows * cols), BF),
            jax.ShapeDtypeStruct(pair.shape, BF),
        ),
        in_specs=[SMEM, VMEM, VMEM],
        out_specs=(VMEM, VMEM),
        compiler_params=pltpu.CompilerParams(vmem_limit_bytes=12 << 20),
        name="edges",
    )(valid, pair, tri_in)


def fast_products(edges, ncol, cols):
    count, both, tokens = edges.shape
    total = ncol * cols
    return pl.pallas_call(
        functools.partial(product_kernel, ncol=ncol, cols=cols),
        out_shape=jax.ShapeDtypeStruct((count, both // 2, total // count, total), BF),
        in_specs=[VMEM],
        out_specs=VMEM,
        scratch_shapes=[pltpu.VMEM((ncol // 4, both * (total + 8), 128), F32)],
        compiler_params=pltpu.CompilerParams(vmem_limit_bytes=12 << 20),
        name="products",
    )(edges)


def fast_middle(prod, x, tri_gate, tri_out, bias_w, heads, copies):
    blocks, own, cols, width = x.shape
    total = blocks * cols
    rows = prod.shape[0]
    return pl.pallas_call(
        middle_kernel,
        out_shape=(
            jax.ShapeDtypeStruct((own, total, width), F32),
            jax.ShapeDtypeStruct((own, total, width), BF),
            jax.ShapeDtypeStruct((copies, heads, own, total), BF),
        ),
        in_specs=[VMEM] * 5,
        out_specs=(VMEM,) * 3,
        scratch_shapes=[
            pltpu.VMEM((total // 128, rows, 128), F32),
            pltpu.VMEM((heads, own, total), F32),
        ],
        compiler_params=pltpu.CompilerParams(vmem_limit_bytes=16 << 20),
        name="middle",
    )(prod, x, tri_gate, tri_out, bias_w)


def fast_project(nm, weights, heads):
    own, total, width = nm.shape
    turned = (own, width, total)
    scale = LOG2E * (width // heads) ** (-0.5)
    return pl.pallas_call(
        functools.partial(project_kernel, scale=scale),
        out_shape=(
            jax.ShapeDtypeStruct(nm.shape, BF),
            jax.ShapeDtypeStruct(nm.shape, BF),
            jax.ShapeDtypeStruct(turned, BF),
            jax.ShapeDtypeStruct(turned, F32),
        ),
        in_specs=[VMEM] * 2,
        out_specs=(VMEM,) * 4,
        cost_estimate=cost(8 * own * total * width * width, 16 * own * total * width),
        compiler_params=pltpu.CompilerParams(vmem_limit_bytes=12 << 20),
        name="project",
    )(nm, weights)


def fast_attention(valid, q, k, v, g, upd, mine, other, wo, cols):
    own, total, width = q.shape
    heads = mine.shape[1]
    blocks = total // cols
    return pl.pallas_call(
        attention_kernel,
        out_shape=jax.ShapeDtypeStruct((blocks, own, cols, width), BF),
        in_specs=[SMEM] + [VMEM] * 8,
        out_specs=VMEM,
        scratch_shapes=[pltpu.VMEM((heads, total, total), F32)] * 2
        + [
            pltpu.VMEM((GROUP * heads, total, total), F32),
            pltpu.VMEM((GROUP * heads, total, total), BF),
        ],
        compiler_params=pltpu.CompilerParams(vmem_limit_bytes=20 << 20),
        name="attention",
    )(valid, q, k, v, g, upd, mine, other, wo)


def plain_edges(valid, pair, tri_in, chans):
    rows, cols, width = pair.shape
    half = tri_in.shape[1] // 2
    parts = jnp.transpose(tri_in).reshape(4, -1, chans, width)
    gates = jnp.stack([parts[0], parts[2]], axis=1)
    vals = jnp.stack([parts[1], parts[3]], axis=1)
    weights = jnp.concatenate([gates.reshape(-1, width), vals.reshape(-1, width)], axis=0)
    row_start = lax.axis_index("row") * rows
    col_start = lax.axis_index(("z", "core")) * cols
    normed = layer_norm(pair).astype(BF)
    proj = jnp.einsum("ec,ikc->eik", weights, normed, preferred_element_type=F32)
    keep_k = (col_start + jnp.arange(cols) < valid[0]).astype(F32)
    keep_i = (row_start + jnp.arange(rows) < valid[0]).astype(F32)
    edge = sigmoid(proj[:half]) * proj[half:] * (keep_i[:, None] * keep_k[None, :])
    return edge.astype(BF).reshape(half, rows * cols), pair.astype(BF)


def plain_products(edges, ncol, cols):
    count, both, tokens = edges.shape
    chans, total = both // 2, ncol * cols
    flat = edges.reshape(count // ncol, ncol, 2, chans, tokens // cols, cols)
    flat = jnp.transpose(flat, (2, 3, 0, 4, 1, 5)).reshape(2, chans, total, total)
    prod = jnp.einsum("cik,cjk->cij", flat[0], flat[1], preferred_element_type=F32).astype(BF)
    return jnp.transpose(prod.reshape(chans, count, total // count, total), (1, 0, 2, 3))


def plain_middle(prod, x, tri_gate, tri_out, bias_w, heads, copies):
    blocks, own, cols, width = x.shape
    total = blocks * cols
    prod = prod.reshape(tri_out.shape[0], own, total).astype(F32)
    nprod = layer_norm(prod, axis=0).astype(BF)
    tri = jnp.einsum("cij,cd->ijd", nprod, tri_out, preferred_element_type=F32)
    pair = jnp.swapaxes(x, 0, 1).reshape(own, total, width).astype(F32)
    normed = layer_norm(pair).astype(BF)
    update = sigmoid(jnp.dot(normed, tri_gate, preferred_element_type=F32)) * tri
    nm = layer_norm(pair + update).astype(BF)
    bias = jnp.einsum("hc,ijc->hij", bias_w[:heads], nm, preferred_element_type=F32).astype(BF)
    return update, nm, jnp.broadcast_to(bias[None], (copies,) + bias.shape)


def plain_project(nm, weights, heads):
    own, total, width = nm.shape
    wqk = weights[:, : 2 * width]
    wvg = jnp.transpose(weights[:, 2 * width :])
    scale = LOG2E * (width // heads) ** (-0.5)
    qk = jnp.dot(nm, wqk, preferred_element_type=F32)
    vg = jnp.einsum("ec,ijc->iej", wvg, nm, preferred_element_type=F32)
    query = (qk[..., :width] * scale).astype(BF)
    return query, qk[..., width:].astype(BF), vg[:, :width].astype(BF), sigmoid(vg[:, width:])


def plain_attention(valid, q, k, v, g, upd, mine, other, wo, cols):
    own, total, width = q.shape
    heads = mine.shape[1]
    size = width // heads
    first = jnp.where(lax.axis_index("core") == 0, mine, other)
    second = jnp.where(lax.axis_index("core") == 0, other, mine)
    table = jnp.stack([first, second], axis=1).astype(F32)
    table = jnp.moveaxis(table, 2, 0).reshape(heads, total, total) * LOG2E
    mask = jnp.where(jnp.arange(total) < valid[0], 0.0, -1000000000.0 * LOG2E).astype(F32)

    def one(args):
        q, k, v = args
        s = jnp.einsum("jhd,khd->hjk", q, k, preferred_element_type=F32) + table + mask
        p = jnp.exp2(s - jnp.max(s, axis=-1, keepdims=True))
        o = jnp.einsum("hjk,hdk->hdj", p.astype(BF), v, preferred_element_type=F32)
        return o / jnp.sum(p, axis=-1)[:, None, :]

    split = (own, total, heads, size)
    v = v.reshape(own, heads, size, total)
    att = lax.map(one, (q.reshape(split), k.reshape(split), v)).reshape(own, width, total)
    gated = (g * att).astype(BF)
    delta = upd + jnp.einsum("icj,cd->ijd", gated, wo, preferred_element_type=F32)
    return jnp.swapaxes(delta.astype(BF).reshape(own, total // cols, cols, width), 0, 1)


def per_device(pair, valid_length, tri_in, tri_gate, tri_out, att_in, att_bias, att_out):
    rows_dev, cols_dev, width = pair.shape
    hidden = tri_out.shape[0]
    heads = att_bias.shape[1]
    col = ("z", "core")
    both = ("row", "z", "core")
    chips = ("row", "z")
    ncol = lax.axis_size("z") * lax.axis_size("core")
    ndev = ncol * lax.axis_size("row")
    total = cols_dev * ncol
    own = rows_dev // ncol
    chans = hidden // ndev
    fast = own % 8 == 0 and total % 128 == 0 and chans == 4 and cols_dev == 32 and ncol % 4 == 0
    edges_of = fast_edges if fast else plain_edges
    products_of = fast_products if fast else plain_products
    middle_of = fast_middle if fast else plain_middle
    project_of = fast_project if fast else plain_project
    attention_of = fast_attention if fast else plain_attention

    edges, xb = edges_of(valid_length, pair, tri_in, chans)
    edges = edges.reshape(ndev, 2 * chans, rows_dev * cols_dev)
    edges = lax.all_to_all(edges, both, 0, 0, tiled=True)
    x = lax.all_to_all(xb, col, 0, 0, tiled=True)
    x = x.reshape(ncol, own, cols_dev, width)
    prod = products_of(edges, ncol, cols_dev)
    prod = prod.reshape(ndev, chans * own, total)
    prod = lax.all_to_all(prod, both, 0, 0, tiled=True).reshape(hidden * own, total)
    bias_w = jnp.pad(jnp.transpose(att_bias), ((0, -heads % 8), (0, 0)))
    upd, nm, bias = middle_of(prod, x, tri_gate, tri_out, bias_w, heads, ndev // 2)
    mine = lax.all_to_all(bias, chips, 0, 0, tiled=True)
    other = lax.ppermute(mine, "core", [(0, 1), (1, 0)])
    q, k, v, g = project_of(nm, att_in, heads)
    delta = attention_of(valid_length, q, k, v, g, upd, mine, other, att_out, cols_dev)
    delta = delta.reshape(rows_dev, cols_dev, width)
    delta = lax.all_to_all(delta, col, 0, 0, tiled=True)
    return pair + delta.astype(F32)


def solution(mesh):
    nrow, ncol = mesh.devices.shape
    split = Mesh(mesh.devices.reshape(nrow, ncol // 2, 2), ("row", "z", "core"))
    home = P("row", ("z", "core"), None)
    placed = (home, P(), P(), P(), P(), P(), P(), P())
    return jax.shard_map(
        per_device, mesh=split, in_specs=placed, out_specs=home, check_vma=False
    )
```

```python
import functools

import jax
import jax.numpy as jnp
from jax import lax
from jax.experimental import pallas as pl
from jax.experimental.pallas import tpu as pltpu
from jax.sharding import Mesh
from jax.sharding import PartitionSpec as P


BF = jnp.bfloat16
F32 = jnp.float32
LOG2E = 1.4426950408889634
GROUP = 2
NT = (((1,), (1,)), ((), ()))
TN = (((0,), (0,)), ((), ()))
NN = (((1,), (0,)), ((), ()))


def mm(a, b, dims):
    return lax.dot_general(a, b, dims, preferred_element_type=F32)


def sigmoid(v):
    return 0.5 * jnp.tanh(0.5 * v) + 0.5


def layer_norm(v, axis=-1):
    center = v - jnp.mean(v, axis=axis, keepdims=True)
    return center * lax.rsqrt(jnp.mean(center * center, axis=axis, keepdims=True) + 1e-05)


def edge_weights(tri_ref, chans):
    hidden = tri_ref.shape[1] // 4
    new = lax.broadcasted_iota(jnp.int32, (2 * hidden, 2 * hidden), 0)
    old = lax.broadcasted_iota(jnp.int32, (2 * hidden, 2 * hidden), 1)
    side = (new // chans) % 2
    wanted = side * hidden + new // (2 * chans) * chans + new % chans
    pick = jnp.where(old == wanted, 1.0, 0.0).astype(BF)
    tri = [tri_ref[:, n * hidden : (n + 1) * hidden] for n in range(4)]
    gates = mm(pick, jnp.concatenate([tri[0], tri[2]], axis=1), NT)
    vals = mm(pick, jnp.concatenate([tri[1], tri[3]], axis=1), NT)
    return jnp.concatenate([gates, vals], axis=0).astype(BF)


def edges_kernel(valid_ref, x_ref, tri_ref, out_ref, *piece_refs, chans):
    rows, cols, width = x_ref.shape
    half = out_ref.shape[0]
    step = 16
    span = step * cols
    valid = valid_ref[0]
    row_start = lax.axis_index("row") * rows
    me = lax.axis_index("z") * 2 + lax.axis_index("core")
    col_start = me * cols
    weights = edge_weights(tri_ref, chans)
    own = rows // len(piece_refs)
    for o, piece in enumerate(piece_refs):
        piece[...] = x_ref[pl.ds((me ^ o) * own, own)].astype(BF)
    token = lax.broadcasted_iota(jnp.int32, (1, span), 1)
    keep_k = (col_start + token % cols < valid).astype(F32)
    for n in range(rows // step):
        x = x_ref[n * step : (n + 1) * step]
        normed = layer_norm(x.reshape(span, width)).astype(BF)
        keep_i = (row_start + n * step + token // cols < valid).astype(F32)
        proj = mm(weights, normed, NT)
        edge = sigmoid(proj[:half]) * proj[half:] * (keep_k * keep_i)
        out_ref[:, n * span : (n + 1) * span] = edge.astype(BF)


def product_kernel(e_ref, out_ref, acc_ref, *, ncol, cols):
    count, both, tokens = e_ref.shape
    chans = both // 2
    quads = ncol // 4
    total = ncol * cols
    rows = tokens // cols
    pitch = acc_ref.shape[1] // both
    lane = lax.broadcasted_iota(jnp.int32, (both, 128), 1)
    low = lane < 64
    even = (lane // 32) % 2 == 0

    def per_row(r, carry):
        for q in range(quads):
            src = [e_ref[r * ncol + q * 4 + g].astype(F32) for g in range(4)]
            for t in range(tokens // 128):
                a = [v[:, t * 128 : (t + 1) * 128] for v in src]
                c = [
                    jnp.where(low, a[0], pltpu.roll(a[2], 64, 1)),
                    jnp.where(low, a[1], pltpu.roll(a[3], 64, 1)),
                    jnp.where(low, pltpu.roll(a[0], 64, 1), a[2]),
                    jnp.where(low, pltpu.roll(a[1], 64, 1), a[3]),
                ]
                d = [
                    jnp.where(even, c[0], pltpu.roll(c[1], 32, 1)),
                    jnp.where(even, pltpu.roll(c[0], 96, 1), c[1]),
                    jnp.where(even, c[2], pltpu.roll(c[3], 32, 1)),
                    jnp.where(even, pltpu.roll(c[2], 96, 1), c[3]),
                ]
                for g in range(4):
                    acc_ref[q, pl.ds(r * rows + t * 4 + g, both, stride=pitch), :] = d[g]
        return carry

    lax.fori_loop(0, count // ncol, per_row, 0)

    def whole(row):
        parts = [acc_ref[q, row * pitch : row * pitch + total, :] for q in range(quads)]
        return jnp.concatenate(parts, axis=1).astype(BF)

    for c in range(chans):
        prod = mm(whole(c), whole(chans + c), NT)
        out_ref[:, c] = prod.reshape(count, total // count, total).astype(BF)


def middle_kernel(p_ref, gate_ref, tri_ref, bias_ref, *refs):
    pieces, (upd_ref, nm_ref, b_ref, acc_ref, bacc_ref, x_ref) = refs[:-6], refs[-6:]
    blocks, own, cols, width = x_ref.shape
    me = lax.axis_index("z") * 2 + lax.axis_index("core")
    for o, piece in enumerate(pieces):
        x_ref[me ^ o] = piece[...]
    total = blocks * cols
    hidden = tri_ref.shape[0]
    heads = b_ref.shape[1]
    for t in range(total // 128):
        acc_ref[t] = p_ref[:, t * 128 : (t + 1) * 128].astype(F32)
    for i in range(own):
        prod = jnp.concatenate(
            [acc_ref[t, pl.ds(i, hidden, stride=own), :] for t in range(total // 128)], axis=1
        )
        nprod = layer_norm(prod, axis=0).astype(BF)
        tri = mm(nprod, tri_ref[...], TN)
        x = x_ref[:, i].reshape(total, width).astype(F32)
        normed = layer_norm(x).astype(BF)
        update = sigmoid(mm(normed, gate_ref[...], NN)) * tri
        nm = layer_norm(x + update).astype(BF)
        upd_ref[i] = update
        nm_ref[i] = nm
        bias = mm(bias_ref[...], nm, NT)
        for h in range(heads):
            bacc_ref[h, i : i + 1, :] = bias[h : h + 1]
    bias = bacc_ref[...].astype(BF)
    for n in range(b_ref.shape[0]):
        b_ref[n] = bias


def project_kernel(nm_ref, w_ref, q_ref, k_ref, v_ref, g_ref, *, scale):
    own, _, width = nm_ref.shape
    turned = jnp.transpose(w_ref[:, 2 * width :].astype(F32)).astype(BF)
    for i in range(own):
        nm = nm_ref[i]
        qk = mm(nm, w_ref[:, : 2 * width], NN)
        q_ref[i] = (qk[:, :width] * scale).astype(BF)
        k_ref[i] = qk[:, width:].astype(BF)
        vg = mm(turned, nm, NT)
        v_ref[i] = vg[:width].astype(BF)
        g_ref[i] = sigmoid(vg[width:])


def attention_kernel(
    valid_ref, q_ref, k_ref, v_ref, g_ref, upd_ref, ba_ref, bb_ref, wo_ref, out_ref, bt_ref, tmp_ref, s_ref, p_ref
):
    count, heads, own, total = ba_ref.shape
    width = wo_ref.shape[0]
    size = width // heads
    blocks, _, cols, _ = out_ref.shape
    group = s_ref.shape[0] // heads
    core = lax.axis_index("core")
    keep = lax.broadcasted_iota(jnp.int32, (total, 1), 0) < valid_ref[0]
    mask = jnp.where(keep, 0.0, -1000000000.0 * LOG2E).astype(F32)
    for h in range(heads):
        for n in range(count):
            for ref, side in ((ba_ref, core), (bb_ref, 1 - core)):
                at = pl.multiple_of((2 * n + side) * own, own)
                tmp_ref[h, pl.ds(at, own), :] = ref[n, h].astype(F32)
        bt_ref[h] = jnp.transpose(tmp_ref[h]) * LOG2E + mask
    lane = lax.broadcasted_iota(jnp.int32, (1, width), 1) // size

    def per_group(n, carry):
        tops = []
        norms = []
        for r in range(group):
            query = q_ref[n * group + r]
            for h in range(heads):
                q = jnp.where(lane == h, query, jnp.zeros_like(query))
                s = mm(k_ref[n * group + r], q, NT) + bt_ref[h]
                s_ref[r * heads + h] = s
                tops.append(jnp.max(s, axis=0, keepdims=True))
        for at in range(group * heads):
            p = jnp.exp2(s_ref[at] - tops[at])
            norms.append(1.0 / jnp.sum(p, axis=0, keepdims=True))
            p_ref[at] = p.astype(BF)
        for r in range(group):
            i = n * group + r
            outs = []
            for h in range(heads):
                at = r * heads + h
                outs.append(mm(v_ref[i, h * size : (h + 1) * size], p_ref[at], NN) * norms[at])
            gated = (jnp.concatenate(outs, axis=0) * g_ref[i]).astype(BF)
            delta = upd_ref[i] + mm(gated, wo_ref[...], TN)
            out_ref[:, pl.ds(i, 1)] = delta.reshape(blocks, 1, cols, width).astype(BF)
        return carry

    lax.fori_loop(0, own // group, per_group, 0)


VMEM = pl.BlockSpec(memory_space=pltpu.VMEM)
SMEM = pl.BlockSpec(memory_space=pltpu.SMEM)


def cost(flops, nbytes):
    return pl.CostEstimate(flops=flops, bytes_accessed=nbytes, transcendentals=0)


def fast_edges(valid, pair, tri_in, chans, ncol):
    rows, cols, width = pair.shape
    half = tri_in.shape[1] // 2
    return pl.pallas_call(
        functools.partial(edges_kernel, chans=chans),
        out_shape=(
            jax.ShapeDtypeStruct((half, rows * cols), BF),
            *[jax.ShapeDtypeStruct((rows // ncol, cols, width), BF)] * ncol,
        ),
        in_specs=[SMEM, VMEM, VMEM],
        out_specs=(VMEM,) * (ncol + 1),
        compiler_params=pltpu.CompilerParams(vmem_limit_bytes=12 << 20),
        name="edges",
    )(valid, pair, tri_in)


def fast_products(edges, ncol, cols):
    count, both, _ = edges.shape
    total = ncol * cols
    return pl.pallas_call(
        functools.partial(product_kernel, ncol=ncol, cols=cols),
        out_shape=jax.ShapeDtypeStruct((count, both // 2, total // count, total), BF),
        in_specs=[VMEM],
        out_specs=VMEM,
        scratch_shapes=[pltpu.VMEM((ncol // 4, both * (total + 8), 128), F32)],
        compiler_params=pltpu.CompilerParams(vmem_limit_bytes=12 << 20),
        name="products",
    )(edges)


def fast_middle(prod, pieces, tri_gate, tri_out, bias_w, heads, copies):
    blocks = len(pieces)
    own, cols, width = pieces[0].shape
    total = blocks * cols
    rows = prod.shape[0]
    return pl.pallas_call(
        middle_kernel,
        out_shape=(
            jax.ShapeDtypeStruct((own, total, width), F32),
            jax.ShapeDtypeStruct((own, total, width), BF),
            jax.ShapeDtypeStruct((copies, heads, own, total), BF),
        ),
        in_specs=[VMEM] * (4 + blocks),
        out_specs=(VMEM,) * 3,
        scratch_shapes=[
            pltpu.VMEM((total // 128, rows, 128), F32),
            pltpu.VMEM((heads, own, total), F32),
            pltpu.VMEM((blocks, own, cols, width), BF),
        ],
        compiler_params=pltpu.CompilerParams(vmem_limit_bytes=16 << 20),
        name="middle",
    )(prod, tri_gate, tri_out, bias_w, *pieces)


def fast_project(nm, weights, heads):
    own, total, width = nm.shape
    turned = (own, width, total)
    scale = LOG2E * (width // heads) ** (-0.5)
    return pl.pallas_call(
        functools.partial(project_kernel, scale=scale),
        out_shape=(
            jax.ShapeDtypeStruct(nm.shape, BF),
            jax.ShapeDtypeStruct(nm.shape, BF),
            jax.ShapeDtypeStruct(turned, BF),
            jax.ShapeDtypeStruct(turned, F32),
        ),
        in_specs=[VMEM] * 2,
        out_specs=(VMEM,) * 4,
        cost_estimate=cost(8 * own * total * width * width, 16 * own * total * width),
        compiler_params=pltpu.CompilerParams(vmem_limit_bytes=12 << 20),
        name="project",
    )(nm, weights)


def fast_attention(valid, q, k, v, g, upd, mine, other, wo, cols):
    own, total, width = q.shape
    heads = mine.shape[1]
    blocks = total // cols
    return pl.pallas_call(
        attention_kernel,
        out_shape=jax.ShapeDtypeStruct((blocks, own, cols, width), BF),
        in_specs=[SMEM] + [VMEM] * 8,
        out_specs=VMEM,
        scratch_shapes=[pltpu.VMEM((heads, total, total), F32)] * 2
        + [
            pltpu.VMEM((GROUP * heads, total, total), F32),
            pltpu.VMEM((GROUP * heads, total, total), BF),
        ],
        compiler_params=pltpu.CompilerParams(vmem_limit_bytes=20 << 20),
        name="attention",
    )(valid, q, k, v, g, upd, mine, other, wo)


def plain_edges(valid, pair, tri_in, chans, ncol):
    rows, cols, width = pair.shape
    half = tri_in.shape[1] // 2
    parts = jnp.transpose(tri_in).reshape(4, -1, chans, width)
    gates = jnp.stack([parts[0], parts[2]], axis=1)
    vals = jnp.stack([parts[1], parts[3]], axis=1)
    weights = jnp.concatenate([gates.reshape(-1, width), vals.reshape(-1, width)], axis=0)
    row_start = lax.axis_index("row") * rows
    col_start = lax.axis_index(("z", "core")) * cols
    normed = layer_norm(pair).astype(BF)
    proj = jnp.einsum("ec,ikc->eik", weights, normed, preferred_element_type=F32)
    keep_k = (col_start + jnp.arange(cols) < valid[0]).astype(F32)
    keep_i = (row_start + jnp.arange(rows) < valid[0]).astype(F32)
    edge = sigmoid(proj[:half]) * proj[half:] * (keep_i[:, None] * keep_k[None, :])
    return edge.astype(BF).reshape(half, rows * cols), pair.astype(BF)


def plain_products(edges, ncol, cols):
    count, both, tokens = edges.shape
    chans, total = both // 2, ncol * cols
    flat = edges.reshape(count // ncol, ncol, 2, chans, tokens // cols, cols)
    flat = jnp.transpose(flat, (2, 3, 0, 4, 1, 5)).reshape(2, chans, total, total)
    prod = jnp.einsum("cik,cjk->cij", flat[0], flat[1], preferred_element_type=F32).astype(BF)
    return jnp.transpose(prod.reshape(chans, count, total // count, total), (1, 0, 2, 3))


def plain_middle(prod, pieces, tri_gate, tri_out, bias_w, heads, copies):
    (x,) = pieces
    blocks, own, cols, width = x.shape
    total = blocks * cols
    prod = prod.reshape(tri_out.shape[0], own, total).astype(F32)
    nprod = layer_norm(prod, axis=0).astype(BF)
    tri = jnp.einsum("cij,cd->ijd", nprod, tri_out, preferred_element_type=F32)
    pair = jnp.swapaxes(x, 0, 1).reshape(own, total, width).astype(F32)
    normed = layer_norm(pair).astype(BF)
    update = sigmoid(jnp.dot(normed, tri_gate, preferred_element_type=F32)) * tri
    nm = layer_norm(pair + update).astype(BF)
    bias = jnp.einsum("hc,ijc->hij", bias_w[:heads], nm, preferred_element_type=F32).astype(BF)
    return update, nm, jnp.broadcast_to(bias[None], (copies,) + bias.shape)


def plain_project(nm, weights, heads):
    _, _, width = nm.shape
    wqk = weights[:, : 2 * width]
    wvg = jnp.transpose(weights[:, 2 * width :])
    scale = LOG2E * (width // heads) ** (-0.5)
    qk = jnp.dot(nm, wqk, preferred_element_type=F32)
    vg = jnp.einsum("ec,ijc->iej", wvg, nm, preferred_element_type=F32)
    query = (qk[..., :width] * scale).astype(BF)
    return query, qk[..., width:].astype(BF), vg[:, :width].astype(BF), sigmoid(vg[:, width:])


def plain_attention(valid, q, k, v, g, upd, mine, other, wo, cols):
    own, total, width = q.shape
    heads = mine.shape[1]
    size = width // heads
    first = jnp.where(lax.axis_index("core") == 0, mine, other)
    second = jnp.where(lax.axis_index("core") == 0, other, mine)
    table = jnp.stack([first, second], axis=1).astype(F32)
    table = jnp.moveaxis(table, 2, 0).reshape(heads, total, total) * LOG2E
    mask = jnp.where(jnp.arange(total) < valid[0], 0.0, -1000000000.0 * LOG2E).astype(F32)

    def one(args):
        q, k, v = args
        s = jnp.einsum("jhd,khd->hjk", q, k, preferred_element_type=F32) + table + mask
        p = jnp.exp2(s - jnp.max(s, axis=-1, keepdims=True))
        o = jnp.einsum("hjk,hdk->hdj", p.astype(BF), v, preferred_element_type=F32)
        return o / jnp.sum(p, axis=-1)[:, None, :]

    split = (own, total, heads, size)
    v = v.reshape(own, heads, size, total)
    att = lax.map(one, (q.reshape(split), k.reshape(split), v)).reshape(own, width, total)
    gated = (g * att).astype(BF)
    delta = upd + jnp.einsum("icj,cd->ijd", gated, wo, preferred_element_type=F32)
    return jnp.swapaxes(delta.astype(BF).reshape(own, total // cols, cols, width), 0, 1)


def per_device(pair, valid_length, tri_in, tri_gate, tri_out, att_in, att_bias, att_out):
    rows_dev, cols_dev, width = pair.shape
    hidden = tri_out.shape[0]
    heads = att_bias.shape[1]
    col = ("z", "core")
    both = ("row", "z", "core")
    chips = ("row", "z")
    ncol = lax.axis_size("z") * lax.axis_size("core")
    ndev = ncol * lax.axis_size("row")
    total = cols_dev * ncol
    own = rows_dev // ncol
    chans = hidden // ndev
    fast = own % 8 == 0 and total % 128 == 0 and chans == 4 and cols_dev == 32 and ncol in (4, 8, 16)
    edges_of = fast_edges if fast else plain_edges
    products_of = fast_products if fast else plain_products
    middle_of = fast_middle if fast else plain_middle
    project_of = fast_project if fast else plain_project
    attention_of = fast_attention if fast else plain_attention

    edges, *pieces = edges_of(valid_length, pair, tri_in, chans, ncol)
    edges = edges.reshape(ndev, 2 * chans, rows_dev * cols_dev)
    if fast:
        for o in range(1, ncol):
            swap = [(n, n ^ o) for n in range(ncol)]
            pieces[o] = lax.ppermute(pieces[o], col, swap)
    else:
        x = lax.all_to_all(pieces[0], col, 0, 0, tiled=True)
        pieces = [x.reshape(ncol, own, cols_dev, width)]
    edges = lax.all_to_all(edges, both, 0, 0, tiled=True)
    prod = products_of(edges, ncol, cols_dev)
    prod = prod.reshape(ndev, chans * own, total)
    prod = lax.all_to_all(prod, both, 0, 0, tiled=True).reshape(hidden * own, total)
    bias_w = jnp.pad(jnp.transpose(att_bias), ((0, -heads % 8), (0, 0)))
    upd, nm, bias = middle_of(prod, pieces, tri_gate, tri_out, bias_w, heads, ndev // 2)
    mine = lax.all_to_all(bias, chips, 0, 0, tiled=True)
    other = lax.ppermute(mine, "core", [(0, 1), (1, 0)])
    q, k, v, g = project_of(nm, att_in, heads)
    delta = attention_of(valid_length, q, k, v, g, upd, mine, other, att_out, cols_dev)
    delta = delta.reshape(rows_dev, cols_dev, width)
    delta = lax.all_to_all(delta, col, 0, 0, tiled=True)
    return pair + delta.astype(F32)


def solution(mesh):
    nrow, ncol = mesh.devices.shape
    split = Mesh(mesh.devices.reshape(nrow, ncol // 2, 2), ("row", "z", "core"))
    home = P("row", ("z", "core"), None)
    placed = (home, P(), P(), P(), P(), P(), P(), P())
    return jax.shard_map(per_device, mesh=split, in_specs=placed, out_specs=home, check_vma=False)
```

```python
import functools

import jax
import jax.numpy as jnp
from jax import lax
from jax.experimental import pallas as pl
from jax.experimental.pallas import tpu as pltpu
from jax.sharding import Mesh
from jax.sharding import PartitionSpec as P


BF = jnp.bfloat16
F32 = jnp.float32
LOG2E = 1.4426950408889634
GROUP = 2
NT = (((1,), (1,)), ((), ()))
TN = (((0,), (0,)), ((), ()))
NN = (((1,), (0,)), ((), ()))


def mm(a, b, dims):
    return lax.dot_general(a, b, dims, preferred_element_type=F32)


def sigmoid(v):
    return 0.5 * jnp.tanh(0.5 * v) + 0.5


def layer_norm(v, axis=-1):
    center = v - jnp.mean(v, axis=axis, keepdims=True)
    return center * lax.rsqrt(jnp.mean(center * center, axis=axis, keepdims=True) + 1e-05)


def edge_weights(tri_ref, chans):
    hidden = tri_ref.shape[1] // 4
    new = lax.broadcasted_iota(jnp.int32, (2 * hidden, 2 * hidden), 0)
    old = lax.broadcasted_iota(jnp.int32, (2 * hidden, 2 * hidden), 1)
    side = (new // chans) % 2
    wanted = side * hidden + new // (2 * chans) * chans + new % chans
    pick = jnp.where(old == wanted, 1.0, 0.0).astype(BF)
    tri = [tri_ref[:, n * hidden : (n + 1) * hidden] for n in range(4)]
    gates = mm(pick, jnp.concatenate([tri[0], tri[2]], axis=1), NT)
    vals = mm(pick, jnp.concatenate([tri[1], tri[3]], axis=1), NT)
    return jnp.concatenate([gates, vals], axis=0).astype(BF)


def edges_kernel(valid_ref, x_ref, tri_ref, out_ref, *piece_refs, chans):
    rows, cols, width = x_ref.shape
    half = out_ref.shape[0]
    step = 16
    span = step * cols
    valid = valid_ref[0]
    row_start = lax.axis_index("row") * rows
    me = lax.axis_index("z") * 2 + lax.axis_index("core")
    col_start = me * cols
    weights = edge_weights(tri_ref, chans)
    own = rows // len(piece_refs)
    for o, piece in enumerate(piece_refs):
        piece[...] = x_ref[pl.ds((me ^ o) * own, own)].astype(BF)
    token = lax.broadcasted_iota(jnp.int32, (1, span), 1)
    keep_k = (col_start + token % cols < valid).astype(F32)
    for n in range(rows // step):
        x = x_ref[n * step : (n + 1) * step]
        normed = layer_norm(x.reshape(span, width)).astype(BF)
        keep_i = (row_start + n * step + token // cols < valid).astype(F32)
        proj = mm(weights, normed, NT)
        edge = sigmoid(proj[:half]) * proj[half:] * (keep_k * keep_i)
        out_ref[:, n * span : (n + 1) * span] = edge.astype(BF)


def product_kernel(e_ref, out_ref, acc_ref, *, ncol, cols):
    count, both, tokens = e_ref.shape
    chans = both // 2
    quads = ncol // 4
    total = ncol * cols
    rows = tokens // cols
    tiles = tokens // 128
    pitch = acc_ref.shape[1] // both
    old = lax.broadcasted_iota(jnp.int32, (512, 512), 0)
    new = lax.broadcasted_iota(jnp.int32, (512, 512), 1)
    wanted = new // 32 % 4 * 128 + new // 128 * 32 + new % 32
    turn = jnp.where(old == wanted, 1.0, 0.0).astype(BF)

    def per_row(r, carry):
        for q in range(quads):
            sides = []
            for g in range(4):
                v = e_ref[r * ncol + q * 4 + g].astype(F32)
                v = [v[:, t * 128 : (t + 1) * 128] for t in range(tiles)]
                sides.append(jnp.concatenate(v, axis=0).astype(BF))
            turned = mm(jnp.concatenate(sides, axis=1), turn, NN)
            for t in range(tiles):
                for g in range(4):
                    part = turned[t * both : (t + 1) * both, g * 128 : (g + 1) * 128]
                    acc_ref[q, pl.ds(r * rows + t * 4 + g, both, stride=pitch), :] = part
        return carry

    lax.fori_loop(0, count // ncol, per_row, 0)

    def whole(row):
        parts = [acc_ref[q, row * pitch : row * pitch + total, :] for q in range(quads)]
        return jnp.concatenate(parts, axis=1).astype(BF)

    for c in range(chans):
        prod = mm(whole(c), whole(chans + c), NT)
        out_ref[:, c] = prod.reshape(count, total // count, total).astype(BF)


def middle_kernel(p_ref, gate_ref, tri_ref, bias_ref, *refs):
    pieces, (upd_ref, nm_ref, b_ref, acc_ref, bacc_ref, x_ref) = refs[:-6], refs[-6:]
    blocks, own, cols, width = x_ref.shape
    me = lax.axis_index("z") * 2 + lax.axis_index("core")
    for o, piece in enumerate(pieces):
        x_ref[me ^ o] = piece[...]
    total = blocks * cols
    hidden = tri_ref.shape[0]
    heads = b_ref.shape[1]
    for t in range(total // 128):
        acc_ref[t] = p_ref[:, t * 128 : (t + 1) * 128].astype(F32)
    for i in range(own):
        prod = jnp.concatenate(
            [acc_ref[t, pl.ds(i, hidden, stride=own), :] for t in range(total // 128)], axis=1
        )
        nprod = layer_norm(prod, axis=0).astype(BF)
        tri = mm(nprod, tri_ref[...], TN)
        x = x_ref[:, i].reshape(total, width).astype(F32)
        normed = layer_norm(x).astype(BF)
        update = sigmoid(mm(normed, gate_ref[...], NN)) * tri
        nm = layer_norm(x + update).astype(BF)
        upd_ref[i] = update
        nm_ref[i] = nm
        bias = mm(bias_ref[...], nm, NT)
        for h in range(heads):
            bacc_ref[h, i : i + 1, :] = bias[h : h + 1]
    bias = bacc_ref[...].astype(BF)
    for n in range(b_ref.shape[0]):
        b_ref[n] = bias


def project_kernel(nm_ref, w_ref, q_ref, k_ref, v_ref, g_ref, *, scale):
    own, _, width = nm_ref.shape
    turned = jnp.transpose(w_ref[:, 2 * width :].astype(F32)).astype(BF)
    for i in range(own):
        nm = nm_ref[i]
        qk = mm(nm, w_ref[:, : 2 * width], NN)
        q_ref[i] = (qk[:, :width] * scale).astype(BF)
        k_ref[i] = qk[:, width:].astype(BF)
        vg = mm(turned, nm, NT)
        v_ref[i] = vg[:width].astype(BF)
        g_ref[i] = sigmoid(vg[width:])


def bias_table(valid_ref, ba_ref, bb_ref, bt_ref, tmp_ref):
    count, heads, own, total = ba_ref.shape
    core = lax.axis_index("core")
    keep = lax.broadcasted_iota(jnp.int32, (total, 1), 0) < valid_ref[0]
    mask = jnp.where(keep, 0.0, -1000000000.0 * LOG2E).astype(F32)
    for h in range(heads):
        for n in range(count):
            for ref, side in ((ba_ref, core), (bb_ref, 1 - core)):
                at = pl.multiple_of((2 * n + side) * own, own)
                tmp_ref[h, pl.ds(at, own), :] = ref[n, h].astype(F32)
        bt_ref[h] = jnp.transpose(tmp_ref[h]) * LOG2E + mask


def attend_rows(q_ref, k_ref, v_ref, g_ref, upd_ref, wo_ref, out_ref, bt_ref, s_ref, p_ref):
    width = wo_ref.shape[0]
    heads = bt_ref.shape[0]
    size = width // heads
    blocks, count, cols, _ = out_ref.shape
    group = s_ref.shape[0] // heads
    lane = lax.broadcasted_iota(jnp.int32, (1, width), 1) // size

    def per_group(n, carry):
        tops = []
        norms = []
        for r in range(group):
            i = n * group + r
            query = q_ref[i]
            for h in range(heads):
                q = jnp.where(lane == h, query, jnp.zeros_like(query))
                s = mm(k_ref[i], q, NT) + bt_ref[h]
                s_ref[r * heads + h] = s
                tops.append(jnp.max(s, axis=0, keepdims=True))
        for at in range(group * heads):
            p = jnp.exp2(s_ref[at] - tops[at])
            norms.append(1.0 / jnp.sum(p, axis=0, keepdims=True))
            p_ref[at] = p.astype(BF)
        for r in range(group):
            i = n * group + r
            outs = []
            for h in range(heads):
                at = r * heads + h
                outs.append(mm(v_ref[i, h * size : (h + 1) * size], p_ref[at], NN) * norms[at])
            gated = (jnp.concatenate(outs, axis=0) * g_ref[i]).astype(BF)
            delta = upd_ref[i] + mm(gated, wo_ref[...], TN)
            out_ref[:, pl.ds(i, 1)] = delta.reshape(blocks, 1, cols, width).astype(BF)
        return carry

    lax.fori_loop(0, count // group, per_group, 0)


def attention_kernel(
    valid_ref, q_ref, k_ref, v_ref, g_ref, upd_ref, ba_ref, bb_ref, wo_ref, *refs
):
    pieces, (out_ref, bt_ref, tmp_ref, s_ref, p_ref) = refs[:-5], refs[-5:]
    bias_table(valid_ref, ba_ref, bb_ref, bt_ref, tmp_ref)
    attend_rows(q_ref, k_ref, v_ref, g_ref, upd_ref, wo_ref, out_ref, bt_ref, s_ref, p_ref)
    me = lax.axis_index("z") * 2 + lax.axis_index("core")
    for o, piece in enumerate(pieces):
        piece[...] = out_ref[me ^ o]


def add_kernel(x_ref, *refs):
    pieces, out_ref = refs[:-1], refs[-1]
    own = pieces[0].shape[0]
    me = lax.axis_index("z") * 2 + lax.axis_index("core")
    for o, piece in enumerate(pieces):
        rows = pl.ds((me ^ o) * own, own)
        out_ref[rows] = x_ref[rows] + piece[...].astype(F32)


VMEM = pl.BlockSpec(memory_space=pltpu.VMEM)
SMEM = pl.BlockSpec(memory_space=pltpu.SMEM)


def cost(flops, nbytes):
    return pl.CostEstimate(flops=flops, bytes_accessed=nbytes, transcendentals=0)


def fast_edges(valid, pair, tri_in, chans, ncol):
    rows, cols, width = pair.shape
    half = tri_in.shape[1] // 2
    return pl.pallas_call(
        functools.partial(edges_kernel, chans=chans),
        out_shape=(
            jax.ShapeDtypeStruct((half, rows * cols), BF),
            *[jax.ShapeDtypeStruct((rows // ncol, cols, width), BF)] * ncol,
        ),
        in_specs=[SMEM, VMEM, VMEM],
        out_specs=(VMEM,) * (ncol + 1),
        compiler_params=pltpu.CompilerParams(vmem_limit_bytes=12 << 20),
        name="edges",
    )(valid, pair, tri_in)


def fast_products(edges, ncol, cols):
    count, both, _ = edges.shape
    total = ncol * cols
    return pl.pallas_call(
        functools.partial(product_kernel, ncol=ncol, cols=cols),
        out_shape=jax.ShapeDtypeStruct((count, both // 2, total // count, total), BF),
        in_specs=[VMEM],
        out_specs=VMEM,
        scratch_shapes=[pltpu.VMEM((ncol // 4, both * (total + 8), 128), F32)],
        compiler_params=pltpu.CompilerParams(vmem_limit_bytes=12 << 20),
        name="products",
    )(edges)


def fast_middle(prod, pieces, tri_gate, tri_out, bias_w, heads, copies):
    blocks = len(pieces)
    own, cols, width = pieces[0].shape
    total = blocks * cols
    rows = prod.shape[0]
    return pl.pallas_call(
        middle_kernel,
        out_shape=(
            jax.ShapeDtypeStruct((own, total, width), F32),
            jax.ShapeDtypeStruct((own, total, width), BF),
            jax.ShapeDtypeStruct((copies, heads, own, total), BF),
        ),
        in_specs=[VMEM] * (4 + blocks),
        out_specs=(VMEM,) * 3,
        scratch_shapes=[
            pltpu.VMEM((total // 128, rows, 128), F32),
            pltpu.VMEM((heads, own, total), F32),
            pltpu.VMEM((blocks, own, cols, width), BF),
        ],
        compiler_params=pltpu.CompilerParams(vmem_limit_bytes=16 << 20),
        name="middle",
    )(prod, tri_gate, tri_out, bias_w, *pieces)


def fast_project(nm, weights, heads):
    own, total, width = nm.shape
    turned = (own, width, total)
    scale = LOG2E * (width // heads) ** (-0.5)
    return pl.pallas_call(
        functools.partial(project_kernel, scale=scale),
        out_shape=(
            jax.ShapeDtypeStruct(nm.shape, BF),
            jax.ShapeDtypeStruct(nm.shape, BF),
            jax.ShapeDtypeStruct(turned, BF),
            jax.ShapeDtypeStruct(turned, F32),
        ),
        in_specs=[VMEM] * 2,
        out_specs=(VMEM,) * 4,
        cost_estimate=cost(8 * own * total * width * width, 16 * own * total * width),
        compiler_params=pltpu.CompilerParams(vmem_limit_bytes=12 << 20),
        name="project",
    )(nm, weights)


def fast_attention(valid, q, k, v, g, upd, mine, other, wo, cols, col):
    own, total, width = q.shape
    heads = mine.shape[1]
    blocks = total // cols
    pieces = pl.pallas_call(
        attention_kernel,
        out_shape=(jax.ShapeDtypeStruct((own, cols, width), BF),) * blocks,
        in_specs=[SMEM] + [VMEM] * 8,
        out_specs=(VMEM,) * blocks,
        scratch_shapes=[
            pltpu.VMEM((blocks, own, cols, width), BF),
            pltpu.VMEM((heads, total, total), F32),
            pltpu.VMEM((heads, total, total), F32),
            pltpu.VMEM((GROUP * heads, total, total), F32),
            pltpu.VMEM((GROUP * heads, total, total), BF),
        ],
        compiler_params=pltpu.CompilerParams(vmem_limit_bytes=20 << 20),
        name="attention",
    )(valid, q, k, v, g, upd, mine, other, wo)
    pieces = list(pieces)
    for o in range(1, blocks):
        pieces[o] = lax.ppermute(pieces[o], col, [(n, n ^ o) for n in range(blocks)])
    return pieces


def fast_add(pair, pieces):
    return pl.pallas_call(
        add_kernel,
        out_shape=jax.ShapeDtypeStruct(pair.shape, F32),
        in_specs=[VMEM] * (1 + len(pieces)),
        out_specs=VMEM,
        compiler_params=pltpu.CompilerParams(vmem_limit_bytes=12 << 20),
        name="add",
    )(pair, *pieces)


def plain_edges(valid, pair, tri_in, chans, ncol):
    rows, cols, width = pair.shape
    half = tri_in.shape[1] // 2
    parts = jnp.transpose(tri_in).reshape(4, -1, chans, width)
    gates = jnp.stack([parts[0], parts[2]], axis=1)
    vals = jnp.stack([parts[1], parts[3]], axis=1)
    weights = jnp.concatenate([gates.reshape(-1, width), vals.reshape(-1, width)], axis=0)
    row_start = lax.axis_index("row") * rows
    col_start = lax.axis_index(("z", "core")) * cols
    normed = layer_norm(pair).astype(BF)
    proj = jnp.einsum("ec,ikc->eik", weights, normed, preferred_element_type=F32)
    keep_k = (col_start + jnp.arange(cols) < valid[0]).astype(F32)
    keep_i = (row_start + jnp.arange(rows) < valid[0]).astype(F32)
    edge = sigmoid(proj[:half]) * proj[half:] * (keep_i[:, None] * keep_k[None, :])
    return edge.astype(BF).reshape(half, rows * cols), pair.astype(BF)


def plain_products(edges, ncol, cols):
    count, both, tokens = edges.shape
    chans, total = both // 2, ncol * cols
    flat = edges.reshape(count // ncol, ncol, 2, chans, tokens // cols, cols)
    flat = jnp.transpose(flat, (2, 3, 0, 4, 1, 5)).reshape(2, chans, total, total)
    prod = jnp.einsum("cik,cjk->cij", flat[0], flat[1], preferred_element_type=F32).astype(BF)
    return jnp.transpose(prod.reshape(chans, count, total // count, total), (1, 0, 2, 3))


def plain_middle(prod, pieces, tri_gate, tri_out, bias_w, heads, copies):
    (x,) = pieces
    blocks, own, cols, width = x.shape
    total = blocks * cols
    prod = prod.reshape(tri_out.shape[0], own, total).astype(F32)
    nprod = layer_norm(prod, axis=0).astype(BF)
    tri = jnp.einsum("cij,cd->ijd", nprod, tri_out, preferred_element_type=F32)
    pair = jnp.swapaxes(x, 0, 1).reshape(own, total, width).astype(F32)
    normed = layer_norm(pair).astype(BF)
    update = sigmoid(jnp.dot(normed, tri_gate, preferred_element_type=F32)) * tri
    nm = layer_norm(pair + update).astype(BF)
    bias = jnp.einsum("hc,ijc->hij", bias_w[:heads], nm, preferred_element_type=F32).astype(BF)
    return update, nm, jnp.broadcast_to(bias[None], (copies,) + bias.shape)


def plain_project(nm, weights, heads):
    _, _, width = nm.shape
    wqk = weights[:, : 2 * width]
    wvg = jnp.transpose(weights[:, 2 * width :])
    scale = LOG2E * (width // heads) ** (-0.5)
    qk = jnp.dot(nm, wqk, preferred_element_type=F32)
    vg = jnp.einsum("ec,ijc->iej", wvg, nm, preferred_element_type=F32)
    query = (qk[..., :width] * scale).astype(BF)
    return query, qk[..., width:].astype(BF), vg[:, :width].astype(BF), sigmoid(vg[:, width:])


def plain_attention(valid, q, k, v, g, upd, mine, other, wo, cols):
    own, total, width = q.shape
    heads = mine.shape[1]
    size = width // heads
    first = jnp.where(lax.axis_index("core") == 0, mine, other)
    second = jnp.where(lax.axis_index("core") == 0, other, mine)
    table = jnp.stack([first, second], axis=1).astype(F32)
    table = jnp.moveaxis(table, 2, 0).reshape(heads, total, total) * LOG2E
    mask = jnp.where(jnp.arange(total) < valid[0], 0.0, -1000000000.0 * LOG2E).astype(F32)

    def one(args):
        q, k, v = args
        s = jnp.einsum("jhd,khd->hjk", q, k, preferred_element_type=F32) + table + mask
        p = jnp.exp2(s - jnp.max(s, axis=-1, keepdims=True))
        o = jnp.einsum("hjk,hdk->hdj", p.astype(BF), v, preferred_element_type=F32)
        return o / jnp.sum(p, axis=-1)[:, None, :]

    split = (own, total, heads, size)
    v = v.reshape(own, heads, size, total)
    att = lax.map(one, (q.reshape(split), k.reshape(split), v)).reshape(own, width, total)
    gated = (g * att).astype(BF)
    delta = upd + jnp.einsum("icj,cd->ijd", gated, wo, preferred_element_type=F32)
    return jnp.swapaxes(delta.astype(BF).reshape(own, total // cols, cols, width), 0, 1)


def per_device(pair, valid_length, tri_in, tri_gate, tri_out, att_in, att_bias, att_out):
    rows_dev, cols_dev, width = pair.shape
    hidden = tri_out.shape[0]
    heads = att_bias.shape[1]
    col = ("z", "core")
    both = ("row", "z", "core")
    chips = ("row", "z")
    ncol = lax.axis_size("z") * lax.axis_size("core")
    ndev = ncol * lax.axis_size("row")
    total = cols_dev * ncol
    own = rows_dev // ncol
    chans = hidden // ndev
    fast = own % 8 == 0 and total % 128 == 0 and chans == 4 and cols_dev == 32 and ncol in (4, 8, 16)
    edges_of = fast_edges if fast else plain_edges
    products_of = fast_products if fast else plain_products
    middle_of = fast_middle if fast else plain_middle
    project_of = fast_project if fast else plain_project

    edges, *pieces = edges_of(valid_length, pair, tri_in, chans, ncol)
    edges = edges.reshape(ndev, 2 * chans, rows_dev * cols_dev)
    if fast:
        for o in range(1, ncol):
            swap = [(n, n ^ o) for n in range(ncol)]
            pieces[o] = lax.ppermute(pieces[o], col, swap)
    else:
        x = lax.all_to_all(pieces[0], col, 0, 0, tiled=True)
        pieces = [x.reshape(ncol, own, cols_dev, width)]
    edges = lax.all_to_all(edges, both, 0, 0, tiled=True)
    prod = products_of(edges, ncol, cols_dev)
    prod = prod.reshape(ndev, chans * own, total)
    prod = lax.all_to_all(prod, both, 0, 0, tiled=True).reshape(hidden * own, total)
    bias_w = jnp.pad(jnp.transpose(att_bias), ((0, -heads % 8), (0, 0)))
    upd, nm, bias = middle_of(prod, pieces, tri_gate, tri_out, bias_w, heads, ndev // 2)
    mine = lax.all_to_all(bias, chips, 0, 0, tiled=True)
    other = lax.ppermute(mine, "core", [(0, 1), (1, 0)])
    q, k, v, g = project_of(nm, att_in, heads)
    if fast:
        pieces = fast_attention(
            valid_length, q, k, v, g, upd, mine, other, att_out, cols_dev, col
        )
        return fast_add(pair, pieces)
    delta = plain_attention(valid_length, q, k, v, g, upd, mine, other, att_out, cols_dev)
    delta = delta.reshape(rows_dev, cols_dev, width)
    delta = lax.all_to_all(delta, col, 0, 0, tiled=True)
    return pair + delta.astype(F32)


def solution(mesh):
    nrow, ncol = mesh.devices.shape
    split = Mesh(mesh.devices.reshape(nrow, ncol // 2, 2), ("row", "z", "core"))
    home = P("row", ("z", "core"), None)
    placed = (home, P(), P(), P(), P(), P(), P(), P())
    return jax.shard_map(per_device, mesh=split, in_specs=placed, out_specs=home, check_vma=False)
```

```python
import functools

import jax
import jax.numpy as jnp
from jax import lax
from jax.experimental import pallas as pl
from jax.experimental.pallas import tpu as pltpu
from jax.sharding import Mesh
from jax.sharding import PartitionSpec as P


BF = jnp.bfloat16
F32 = jnp.float32
LOG2E = 1.4426950408889634
GROUP = 8
NT = (((1,), (1,)), ((), ()))
TN = (((0,), (0,)), ((), ()))
NN = (((1,), (0,)), ((), ()))


def mm(a, b, dims):
    return lax.dot_general(a, b, dims, preferred_element_type=F32)


def sigmoid(v):
    return 0.5 * jnp.tanh(0.5 * v) + 0.5


def layer_norm(v, axis=-1):
    center = v - jnp.mean(v, axis=axis, keepdims=True)
    return center * lax.rsqrt(jnp.mean(center * center, axis=axis, keepdims=True) + 1e-05)


def edge_weights(tri_ref, chans):
    hidden = tri_ref.shape[1] // 4
    new = lax.broadcasted_iota(jnp.int32, (2 * hidden, 2 * hidden), 0)
    old = lax.broadcasted_iota(jnp.int32, (2 * hidden, 2 * hidden), 1)
    side = (new // chans) % 2
    wanted = side * hidden + new // (2 * chans) * chans + new % chans
    pick = jnp.where(old == wanted, 1.0, 0.0).astype(BF)
    tri = [tri_ref[:, n * hidden : (n + 1) * hidden] for n in range(4)]
    gates = mm(pick, jnp.concatenate([tri[0], tri[2]], axis=1), NT)
    vals = mm(pick, jnp.concatenate([tri[1], tri[3]], axis=1), NT)
    return jnp.concatenate([gates, vals], axis=0).astype(BF)


def pieces_kernel(x_ref, *piece_refs):
    own = x_ref.shape[0] // len(piece_refs)
    me = lax.axis_index("z") * 2 + lax.axis_index("core")
    for o, piece in enumerate(piece_refs):
        piece[...] = x_ref[pl.ds((me ^ o) * own, own)].astype(BF)


def edges_kernel(valid_ref, x_ref, tri_ref, out_ref, *, chans):
    rows, cols, width = x_ref.shape
    half = out_ref.shape[0]
    step = 16
    span = step * cols
    valid = valid_ref[0]
    row_start = lax.axis_index("row") * rows
    me = lax.axis_index("z") * 2 + lax.axis_index("core")
    col_start = me * cols
    weights = edge_weights(tri_ref, chans)
    token = lax.broadcasted_iota(jnp.int32, (1, span), 1)
    keep_k = (col_start + token % cols < valid).astype(F32)
    for n in range(rows // step):
        x = x_ref[n * step : (n + 1) * step]
        normed = layer_norm(x.reshape(span, width)).astype(BF)
        keep_i = (row_start + n * step + token // cols < valid).astype(F32)
        proj = mm(weights, normed, NT)
        edge = sigmoid(proj[:half]) * proj[half:] * (keep_k * keep_i)
        out_ref[:, n * span : (n + 1) * span] = edge.astype(BF)


def product_kernel(e_ref, out_ref, acc_ref, *, ncol, cols):
    count, both, tokens = e_ref.shape
    chans = both // 2
    quads = ncol // 4
    total = ncol * cols
    rows = tokens // cols
    tiles = tokens // 128
    pitch = acc_ref.shape[1] // both
    old = lax.broadcasted_iota(jnp.int32, (512, 512), 0)
    new = lax.broadcasted_iota(jnp.int32, (512, 512), 1)
    wanted = new // 32 % 4 * 128 + new // 128 * 32 + new % 32
    turn = jnp.where(old == wanted, 1.0, 0.0).astype(BF)

    def per_row(r, carry):
        for q in range(quads):
            sides = []
            for g in range(4):
                v = e_ref[r * ncol + q * 4 + g].astype(F32)
                v = [v[:, t * 128 : (t + 1) * 128] for t in range(tiles)]
                sides.append(jnp.concatenate(v, axis=0).astype(BF))
            turned = mm(jnp.concatenate(sides, axis=1), turn, NN)
            for t in range(tiles):
                for g in range(4):
                    part = turned[t * both : (t + 1) * both, g * 128 : (g + 1) * 128]
                    acc_ref[q, pl.ds(r * rows + t * 4 + g, both, stride=pitch), :] = part
        return carry

    lax.fori_loop(0, count // ncol, per_row, 0)

    def whole(row):
        parts = [acc_ref[q, row * pitch : row * pitch + total, :] for q in range(quads)]
        return jnp.concatenate(parts, axis=1).astype(BF)

    for c in range(chans):
        prod = mm(whole(c), whole(chans + c), NT)
        out_ref[:, c] = prod.reshape(count, total // count, total).astype(BF)


def gate_kernel(gate_ref, *refs):
    pieces, (x_ref, out_ref) = refs[:-2], refs[-2:]
    blocks, own, cols, width = x_ref.shape
    me = lax.axis_index("z") * 2 + lax.axis_index("core")
    for o, piece in enumerate(pieces):
        x_ref[me ^ o] = piece[...]
    for i in range(own):
        x = x_ref[:, i].reshape(blocks * cols, width).astype(F32)
        out_ref[i] = sigmoid(mm(layer_norm(x).astype(BF), gate_ref[...], NN))


def middle_kernel(p_ref, x_ref, g_ref, tri_ref, bias_ref, upd_ref, nm_ref, b_ref, acc_ref, bacc_ref):
    blocks, own, cols, width = x_ref.shape
    total = blocks * cols
    hidden = tri_ref.shape[0]
    heads = b_ref.shape[1]
    for t in range(total // 128):
        acc_ref[t] = p_ref[:, t * 128 : (t + 1) * 128].astype(F32)
    for i in range(own):
        prod = jnp.concatenate(
            [acc_ref[t, pl.ds(i, hidden, stride=own), :] for t in range(total // 128)], axis=1
        )
        nprod = layer_norm(prod, axis=0).astype(BF)
        update = g_ref[i] * mm(nprod, tri_ref[...], TN)
        x = x_ref[:, i].reshape(total, width).astype(F32)
        nm = layer_norm(x + update).astype(BF)
        upd_ref[i] = update
        nm_ref[i] = nm
        bias = mm(bias_ref[...], nm, NT)
        for h in range(heads):
            bacc_ref[h, i : i + 1, :] = bias[h : h + 1]
    bias = bacc_ref[...].astype(BF)
    for n in range(b_ref.shape[0]):
        b_ref[n] = bias


def project_kernel(nm_ref, w_ref, q_ref, k_ref, v_ref, g_ref, *, scale):
    own, _, width = nm_ref.shape
    turned = jnp.transpose(w_ref[:, 2 * width :].astype(F32)).astype(BF)
    for i in range(own):
        nm = nm_ref[i]
        qk = mm(nm, w_ref[:, : 2 * width], NN)
        q_ref[i] = (qk[:, :width] * scale).astype(BF)
        k_ref[i] = qk[:, width:].astype(BF)
        vg = mm(turned, nm, NT)
        v_ref[i] = vg[:width].astype(BF)
        g_ref[i] = sigmoid(vg[width:])


def bias_table(valid_ref, mine_refs, other_refs, bt_ref, tmp_ref):
    nrow, heads, own, total = mine_refs[0].shape
    nz = len(mine_refs)
    row, z, core = lax.axis_index("row"), lax.axis_index("z"), lax.axis_index("core")
    keep = lax.broadcasted_iota(jnp.int32, (total, 1), 0) < valid_ref[0]
    mask = jnp.where(keep, 0.0, -1000000000.0 * LOG2E).astype(F32)
    for h in range(heads):
        for o in range(nz):
            for r in range(nrow):
                chip = (row ^ r) * nz + (z ^ o)
                for refs, side in ((mine_refs, core), (other_refs, 1 - core)):
                    at = pl.multiple_of((2 * chip + side) * own, own)
                    tmp_ref[h, pl.ds(at, own), :] = refs[o][r, h].astype(F32)
        bt_ref[h] = jnp.transpose(tmp_ref[h]) * LOG2E + mask


def attend_rows(q_ref, k_ref, v_ref, g_ref, upd_ref, wo_ref, out_ref, bt_ref, s_ref, p_ref):
    width = wo_ref.shape[0]
    heads = bt_ref.shape[0]
    size = width // heads
    blocks, count, cols, _ = out_ref.shape
    group = s_ref.shape[0] // heads
    lane = lax.broadcasted_iota(jnp.int32, (1, width), 1) // size

    def per_group(n, carry):
        tops = []
        norms = []
        for r in range(group):
            i = n * group + r
            query = q_ref[i]
            for h in range(heads):
                q = jnp.where(lane == h, query, jnp.zeros_like(query))
                s = mm(k_ref[i], q, NT) + bt_ref[h]
                s_ref[r * heads + h] = s
                tops.append(jnp.max(s, axis=0, keepdims=True))
        for at in range(group * heads):
            p = jnp.exp2(s_ref[at] - tops[at])
            norms.append(1.0 / jnp.sum(p, axis=0, keepdims=True))
            p_ref[at] = p.astype(BF)
        for r in range(group):
            i = n * group + r
            outs = []
            for h in range(heads):
                at = r * heads + h
                outs.append(mm(v_ref[i, h * size : (h + 1) * size], p_ref[at], NN) * norms[at])
            gated = (jnp.concatenate(outs, axis=0) * g_ref[i]).astype(BF)
            delta = upd_ref[i] + mm(gated, wo_ref[...], TN)
            out_ref[:, pl.ds(i, 1)] = delta.reshape(blocks, 1, cols, width).astype(BF)
        return carry

    lax.fori_loop(0, count // group, per_group, 0)


def attention_kernel(valid_ref, q_ref, k_ref, v_ref, g_ref, upd_ref, wo_ref, *refs, nz):
    mine_refs, other_refs, refs = refs[:nz], refs[nz : 2 * nz], refs[2 * nz :]
    pieces, (out_ref, bt_ref, tmp_ref, s_ref, p_ref) = refs[:-5], refs[-5:]
    bias_table(valid_ref, mine_refs, other_refs, bt_ref, tmp_ref)
    attend_rows(q_ref, k_ref, v_ref, g_ref, upd_ref, wo_ref, out_ref, bt_ref, s_ref, p_ref)
    me = lax.axis_index("z") * 2 + lax.axis_index("core")
    for o, piece in enumerate(pieces):
        piece[...] = out_ref[me ^ o]


def add_kernel(x_ref, *refs):
    pieces, out_ref = refs[:-1], refs[-1]
    own = pieces[0].shape[0]
    me = lax.axis_index("z") * 2 + lax.axis_index("core")
    for o, piece in enumerate(pieces):
        rows = pl.ds((me ^ o) * own, own)
        out_ref[rows] = x_ref[rows] + piece[...].astype(F32)


VMEM = pl.BlockSpec(memory_space=pltpu.VMEM)
SMEM = pl.BlockSpec(memory_space=pltpu.SMEM)


def cost(flops, nbytes):
    return pl.CostEstimate(flops=flops, bytes_accessed=nbytes, transcendentals=0)


def fast_pieces(pair, ncol):
    rows, cols, width = pair.shape
    return pl.pallas_call(
        pieces_kernel,
        out_shape=(jax.ShapeDtypeStruct((rows // ncol, cols, width), BF),) * ncol,
        in_specs=[VMEM],
        out_specs=(VMEM,) * ncol,
        compiler_params=pltpu.CompilerParams(vmem_limit_bytes=8 << 20),
        name="pieces",
    )(pair)


def fast_edges(valid, pair, tri_in, chans, ncol):
    rows, cols, _ = pair.shape
    half = tri_in.shape[1] // 2
    pieces = fast_pieces(pair, ncol)
    edges = pl.pallas_call(
        functools.partial(edges_kernel, chans=chans),
        out_shape=jax.ShapeDtypeStruct((half, rows * cols), BF),
        in_specs=[SMEM, VMEM, VMEM],
        out_specs=VMEM,
        compiler_params=pltpu.CompilerParams(vmem_limit_bytes=12 << 20),
        name="edges",
    )(valid, pair, tri_in)
    return edges, *pieces


def fast_products(edges, ncol, cols):
    count, both, _ = edges.shape
    total = ncol * cols
    return pl.pallas_call(
        functools.partial(product_kernel, ncol=ncol, cols=cols),
        out_shape=jax.ShapeDtypeStruct((count, both // 2, total // count, total), BF),
        in_specs=[VMEM],
        out_specs=VMEM,
        scratch_shapes=[pltpu.VMEM((ncol // 4, both * (total + 8), 128), F32)],
        compiler_params=pltpu.CompilerParams(vmem_limit_bytes=12 << 20),
        name="products",
    )(edges)


def fast_gate(pieces, tri_gate):
    blocks = len(pieces)
    own, cols, width = pieces[0].shape
    total = blocks * cols
    return pl.pallas_call(
        gate_kernel,
        out_shape=(
            jax.ShapeDtypeStruct((blocks, own, cols, width), BF),
            jax.ShapeDtypeStruct((own, total, width), F32),
        ),
        in_specs=[VMEM] * (1 + blocks),
        out_specs=(VMEM,) * 2,
        compiler_params=pltpu.CompilerParams(vmem_limit_bytes=12 << 20),
        cost_estimate=cost(2 * own * total * width * width, 10 * own * total * width),
        name="gate",
    )(tri_gate, *pieces)


def fast_middle(prod, pieces, tri_gate, tri_out, bias_w, heads, copies):
    x, gate = fast_gate(pieces, tri_gate)
    blocks, own, cols, width = x.shape
    total = blocks * cols
    rows = prod.shape[0]
    return pl.pallas_call(
        middle_kernel,
        out_shape=(
            jax.ShapeDtypeStruct((own, total, width), F32),
            jax.ShapeDtypeStruct((own, total, width), BF),
            jax.ShapeDtypeStruct((copies, heads, own, total), BF),
        ),
        in_specs=[VMEM] * 5,
        out_specs=(VMEM,) * 3,
        scratch_shapes=[
            pltpu.VMEM((total // 128, rows, 128), F32),
            pltpu.VMEM((heads, own, total), F32),
        ],
        compiler_params=pltpu.CompilerParams(vmem_limit_bytes=16 << 20),
        name="middle",
    )(prod, x, gate, tri_out, bias_w)


def fast_project(nm, weights, heads):
    own, total, width = nm.shape
    turned = (own, width, total)
    scale = LOG2E * (width // heads) ** (-0.5)
    return pl.pallas_call(
        functools.partial(project_kernel, scale=scale),
        out_shape=(
            jax.ShapeDtypeStruct(nm.shape, BF),
            jax.ShapeDtypeStruct(nm.shape, BF),
            jax.ShapeDtypeStruct(turned, BF),
            jax.ShapeDtypeStruct(turned, F32),
        ),
        in_specs=[VMEM] * 2,
        out_specs=(VMEM,) * 4,
        cost_estimate=cost(8 * own * total * width * width, 16 * own * total * width),
        compiler_params=pltpu.CompilerParams(vmem_limit_bytes=12 << 20),
        name="project",
    )(nm, weights)


def fast_attention(valid, q, k, v, g, upd, mine, other, wo, cols, col):
    own, total, width = q.shape
    heads = mine[0].shape[1]
    blocks = total // cols
    pieces = pl.pallas_call(
        functools.partial(attention_kernel, nz=len(mine)),
        out_shape=(jax.ShapeDtypeStruct((own, cols, width), BF),) * blocks,
        in_specs=[SMEM] + [VMEM] * (6 + 2 * len(mine)),
        out_specs=(VMEM,) * blocks,
        scratch_shapes=[
            pltpu.VMEM((blocks, own, cols, width), BF),
            pltpu.VMEM((heads, total, total), F32),
            pltpu.VMEM((heads, total, total), F32),
            pltpu.VMEM((GROUP * heads, total, total), F32),
            pltpu.VMEM((GROUP * heads, total, total), BF),
        ],
        compiler_params=pltpu.CompilerParams(vmem_limit_bytes=28 << 20),
        name="attention",
    )(valid, q, k, v, g, upd, wo, *mine, *other)
    pieces = list(pieces)
    for o in range(1, blocks):
        pieces[o] = lax.ppermute(pieces[o], col, [(n, n ^ o) for n in range(blocks)])
    return pieces


def fast_add(pair, pieces):
    return pl.pallas_call(
        add_kernel,
        out_shape=jax.ShapeDtypeStruct(pair.shape, F32),
        in_specs=[VMEM] * (1 + len(pieces)),
        out_specs=VMEM,
        compiler_params=pltpu.CompilerParams(vmem_limit_bytes=12 << 20),
        name="add",
    )(pair, *pieces)


def plain_edges(valid, pair, tri_in, chans, ncol):
    rows, cols, width = pair.shape
    half = tri_in.shape[1] // 2
    parts = jnp.transpose(tri_in).reshape(4, -1, chans, width)
    gates = jnp.stack([parts[0], parts[2]], axis=1)
    vals = jnp.stack([parts[1], parts[3]], axis=1)
    weights = jnp.concatenate([gates.reshape(-1, width), vals.reshape(-1, width)], axis=0)
    row_start = lax.axis_index("row") * rows
    col_start = lax.axis_index(("z", "core")) * cols
    normed = layer_norm(pair).astype(BF)
    proj = jnp.einsum("ec,ikc->eik", weights, normed, preferred_element_type=F32)
    keep_k = (col_start + jnp.arange(cols) < valid[0]).astype(F32)
    keep_i = (row_start + jnp.arange(rows) < valid[0]).astype(F32)
    edge = sigmoid(proj[:half]) * proj[half:] * (keep_i[:, None] * keep_k[None, :])
    return edge.astype(BF).reshape(half, rows * cols), pair.astype(BF)


def plain_products(edges, ncol, cols):
    count, both, tokens = edges.shape
    chans, total = both // 2, ncol * cols
    flat = edges.reshape(count // ncol, ncol, 2, chans, tokens // cols, cols)
    flat = jnp.transpose(flat, (2, 3, 0, 4, 1, 5)).reshape(2, chans, total, total)
    prod = jnp.einsum("cik,cjk->cij", flat[0], flat[1], preferred_element_type=F32).astype(BF)
    return jnp.transpose(prod.reshape(chans, count, total // count, total), (1, 0, 2, 3))


def plain_middle(prod, pieces, tri_gate, tri_out, bias_w, heads, copies):
    (x,) = pieces
    blocks, own, cols, width = x.shape
    total = blocks * cols
    prod = prod.reshape(tri_out.shape[0], own, total).astype(F32)
    nprod = layer_norm(prod, axis=0).astype(BF)
    tri = jnp.einsum("cij,cd->ijd", nprod, tri_out, preferred_element_type=F32)
    pair = jnp.swapaxes(x, 0, 1).reshape(own, total, width).astype(F32)
    normed = layer_norm(pair).astype(BF)
    update = sigmoid(jnp.dot(normed, tri_gate, preferred_element_type=F32)) * tri
    nm = layer_norm(pair + update).astype(BF)
    bias = jnp.einsum("hc,ijc->hij", bias_w[:heads], nm, preferred_element_type=F32).astype(BF)
    return update, nm, jnp.broadcast_to(bias[None], (copies,) + bias.shape)


def plain_project(nm, weights, heads):
    _, _, width = nm.shape
    wqk = weights[:, : 2 * width]
    wvg = jnp.transpose(weights[:, 2 * width :])
    scale = LOG2E * (width // heads) ** (-0.5)
    qk = jnp.dot(nm, wqk, preferred_element_type=F32)
    vg = jnp.einsum("ec,ijc->iej", wvg, nm, preferred_element_type=F32)
    query = (qk[..., :width] * scale).astype(BF)
    return query, qk[..., width:].astype(BF), vg[:, :width].astype(BF), sigmoid(vg[:, width:])


def plain_attention(valid, q, k, v, g, upd, mine, other, wo, cols):
    own, total, width = q.shape
    heads = mine.shape[1]
    size = width // heads
    first = jnp.where(lax.axis_index("core") == 0, mine, other)
    second = jnp.where(lax.axis_index("core") == 0, other, mine)
    table = jnp.stack([first, second], axis=1).astype(F32)
    table = jnp.moveaxis(table, 2, 0).reshape(heads, total, total) * LOG2E
    mask = jnp.where(jnp.arange(total) < valid[0], 0.0, -1000000000.0 * LOG2E).astype(F32)

    def one(args):
        q, k, v = args
        s = jnp.einsum("jhd,khd->hjk", q, k, preferred_element_type=F32) + table + mask
        p = jnp.exp2(s - jnp.max(s, axis=-1, keepdims=True))
        o = jnp.einsum("hjk,hdk->hdj", p.astype(BF), v, preferred_element_type=F32)
        return o / jnp.sum(p, axis=-1)[:, None, :]

    split = (own, total, heads, size)
    v = v.reshape(own, heads, size, total)
    att = lax.map(one, (q.reshape(split), k.reshape(split), v)).reshape(own, width, total)
    gated = (g * att).astype(BF)
    delta = upd + jnp.einsum("icj,cd->ijd", gated, wo, preferred_element_type=F32)
    return jnp.swapaxes(delta.astype(BF).reshape(own, total // cols, cols, width), 0, 1)


def spread(part, axis):
    size = lax.axis_size(axis)
    moves = [[(n, n ^ o) for n in range(size)] for o in range(1, size)]
    return [part] + [lax.ppermute(part, axis, move) for move in moves]


def per_device(pair, valid_length, tri_in, tri_gate, tri_out, att_in, att_bias, att_out):
    rows_dev, cols_dev, width = pair.shape
    hidden = tri_out.shape[0]
    heads = att_bias.shape[1]
    col = ("z", "core")
    both = ("row", "z", "core")
    chips = ("row", "z")
    ncol = lax.axis_size("z") * lax.axis_size("core")
    ndev = ncol * lax.axis_size("row")
    total = cols_dev * ncol
    own = rows_dev // ncol
    chans = hidden // ndev
    fast = own % 8 == 0 and total % 128 == 0 and chans == 4 and cols_dev == 32
    fast = fast and ncol in (4, 8, 16) and lax.axis_size("row") in (2, 4, 8)
    edges_of = fast_edges if fast else plain_edges
    products_of = fast_products if fast else plain_products
    middle_of = fast_middle if fast else plain_middle
    project_of = fast_project if fast else plain_project

    edges, *pieces = edges_of(valid_length, pair, tri_in, chans, ncol)
    edges = edges.reshape(ndev, 2 * chans, rows_dev * cols_dev)
    if fast:
        for o in range(1, ncol):
            swap = [(n, n ^ o) for n in range(ncol)]
            pieces[o] = lax.ppermute(pieces[o], col, swap)
    else:
        x = lax.all_to_all(pieces[0], col, 0, 0, tiled=True)
        pieces = [x.reshape(ncol, own, cols_dev, width)]
    edges = lax.all_to_all(edges, both, 0, 0, tiled=True)
    prod = products_of(edges, ncol, cols_dev)
    prod = prod.reshape(ndev, chans * own, total)
    prod = lax.all_to_all(prod, both, 0, 0, tiled=True).reshape(hidden * own, total)
    bias_w = jnp.pad(jnp.transpose(att_bias), ((0, -heads % 8), (0, 0)))
    upd, nm, bias = middle_of(prod, pieces, tri_gate, tri_out, bias_w, heads, 1 if fast else ndev // 2)
    if fast:
        rows = jnp.stack(spread(bias[0], "row"))
        mine = spread(rows, "z")
        other = [lax.ppermute(part, "core", [(0, 1), (1, 0)]) for part in mine]
    else:
        mine = lax.all_to_all(bias, chips, 0, 0, tiled=True)
        other = lax.ppermute(mine, "core", [(0, 1), (1, 0)])
    q, k, v, g = project_of(nm, att_in, heads)
    if fast:
        pieces = fast_attention(
            valid_length, q, k, v, g, upd, mine, other, att_out, cols_dev, col
        )
        return fast_add(pair, pieces)
    delta = plain_attention(valid_length, q, k, v, g, upd, mine, other, att_out, cols_dev)
    delta = delta.reshape(rows_dev, cols_dev, width)
    delta = lax.all_to_all(delta, col, 0, 0, tiled=True)
    return pair + delta.astype(F32)


def solution(mesh):
    nrow, ncol = mesh.devices.shape
    split = Mesh(mesh.devices.reshape(nrow, ncol // 2, 2), ("row", "z", "core"))
    home = P("row", ("z", "core"), None)
    placed = (home, P(), P(), P(), P(), P(), P(), P())
    return jax.shard_map(per_device, mesh=split, in_specs=placed, out_specs=home, check_vma=False)
```
